16 devices in a mesh: dp: 16 (over z, y, x, core).
Axes of the slice: x: 2, y: 2, z: 2, core: 2. Of those that a mesh axis runs over, the one named last changes fastest.
Arguments:
- user_x: float32 [8192, 384], P('dp')
- item_x: float32 [8192, 384], P('dp')
- item_id: int32 [8192], P('dp')
- log_q: float32 [8192], P('dp')
- user_w1: float32 [384, 1536], replicated
- user_w2: float32 [1536, 384], replicated
- user_w3: float32 [384, 384], replicated
- item_w1: float32 [384, 1536], replicated
- item_w2: float32 [1536, 384], replicated
- item_w3: float32 [384, 384], replicated
Outputs:
- output 1: float32 [], replicated
- output 2: float32 [384, 1536], replicated
- output 3: float32 [1536, 384], replicated
- output 4: float32 [384, 384], replicated
- output 5: float32 [384, 1536], replicated
- output 6: float32 [1536, 384], replicated
- output 7: float32 [384, 384], replicated
All inputs are finite; a program needn't handle non-finite values.
Results may differ from the reference program's by a relative error of at most 0.0042753.
Values are sent between devices in bfloat16 or wider.
A program may use at most 1 GiB of HBM per device.

```python
import jax
import jax.numpy as jnp
from jax import lax

ROWS_DEV = 512
GROUP_SIZE = 16
IN_WIDTH = 384
HIDDEN_A = 1536
HIDDEN_B = 384
EMBED_DIM = 384

BATCH = ROWS_DEV * GROUP_SIZE
ID_RANGE = max(BATCH // 64, 2)
TEMPERATURE = 0.05
INV_TEMP = 1.0 / TEMPERATURE
NORM_EPS = 1e-6


def id_features(key, item_id):
    def one_row(one_id):
        return jax.random.normal(jax.random.fold_in(key, one_id), (IN_WIDTH,), jnp.float32)
    return jax.vmap(one_row)(item_id)


def setup_inputs(seed: int = 0) -> dict:
    keys = jax.random.split(jax.random.key(seed), 12)
    shapes = ((IN_WIDTH, HIDDEN_A), (HIDDEN_A, HIDDEN_B), (HIDDEN_B, EMBED_DIM))
    gains = (2.0, 2.0, 1.0)
    user_ws = []
    item_ws = []
    for layer in range(3):
        scale = (gains[layer] / shapes[layer][0]) ** 0.5
        base = jax.random.normal(keys[layer], shapes[layer], jnp.float32)
        other = jax.random.normal(keys[layer + 3], shapes[layer], jnp.float32)
        user_ws.append(base * scale)
        item_ws.append((0.95 * base + 0.31 * other) * scale)
    item_id = jax.random.randint(keys[6], (BATCH,), 0, ID_RANGE, dtype=jnp.int32)
    item_x = 0.97 * id_features(keys[7], item_id) + 0.243 * jax.random.normal(keys[8], (BATCH, IN_WIDTH), jnp.float32)
    user_x = 0.95 * item_x + 0.31 * jax.random.normal(keys[9], (BATCH, IN_WIDTH), jnp.float32)
    log_q = jax.random.uniform(keys[10], (BATCH,), jnp.float32, -12.0, -6.0)
    return {'user_x': user_x, 'item_x': item_x, 'item_id': item_id, 'log_q': log_q,
            'user_w1': user_ws[0], 'user_w2': user_ws[1], 'user_w3': user_ws[2],
            'item_w1': item_ws[0], 'item_w2': item_ws[1], 'item_w3': item_ws[2]}


def tower_forward(inputs, w_one, w_two, w_three):
    x_half = inputs.astype(jnp.bfloat16)
    pre_one = jnp.dot(x_half, w_one.astype(jnp.bfloat16), preferred_element_type=jnp.float32)
    act_one = jnp.maximum(pre_one, 0.0).astype(jnp.bfloat16)
    pre_two = jnp.dot(act_one, w_two.astype(jnp.bfloat16), preferred_element_type=jnp.float32)
    act_two = jnp.maximum(pre_two, 0.0).astype(jnp.bfloat16)
    raw_out = jnp.dot(act_two, w_three.astype(jnp.bfloat16), preferred_element_type=jnp.float32)
    inv_norm = lax.rsqrt(jnp.sum(raw_out * raw_out, axis=1, keepdims=True) + NORM_EPS)
    return (x_half, pre_one, act_one, pre_two, act_two, raw_out * inv_norm, inv_norm)


def tower_grads(inputs, w_one, w_two, w_three, grad_unit):
    x_half, pre_one, act_one, pre_two, act_two, unit_out, inv_norm = tower_forward(inputs, w_one, w_two, w_three)
    grad_raw = inv_norm * (grad_unit - unit_out * jnp.sum(unit_out * grad_unit, axis=1, keepdims=True))
    grad_raw_h = grad_raw.astype(jnp.bfloat16)
    grad_three = jnp.dot(act_two.T, grad_raw_h, preferred_element_type=jnp.float32)
    grad_act_two = jnp.dot(grad_raw_h, w_three.astype(jnp.bfloat16).T, preferred_element_type=jnp.float32)
    grad_pre_two = jnp.where(pre_two > 0.0, grad_act_two, 0.0).astype(jnp.bfloat16)
    grad_two = jnp.dot(act_one.T, grad_pre_two, preferred_element_type=jnp.float32)
    grad_act_one = jnp.dot(grad_pre_two, w_two.astype(jnp.bfloat16).T, preferred_element_type=jnp.float32)
    grad_pre_one = jnp.where(pre_one > 0.0, grad_act_one, 0.0).astype(jnp.bfloat16)
    grad_one = jnp.dot(x_half.T, grad_pre_one, preferred_element_type=jnp.float32)
    return (grad_one, grad_two, grad_three)


def accumulate_grads(x_shards, grad_shards, w_one, w_two, w_three):
    def grad_step(carry, shard):
        step_grads = tower_grads(shard[0], w_one, w_two, w_three, shard[1])
        return tuple(total + part for total, part in zip(carry, step_grads)), None
    zeros = (jnp.zeros(w_one.shape, jnp.float32), jnp.zeros(w_two.shape, jnp.float32), jnp.zeros(w_three.shape, jnp.float32))
    return lax.scan(grad_step, zeros, (x_shards, grad_shards))[0]


def reference(user_x, item_x, item_id, log_q, user_w1, user_w2, user_w3, item_w1, item_w2, item_w3):
    user_shards = user_x.reshape(GROUP_SIZE, ROWS_DEV, IN_WIDTH)
    item_shards = item_x.reshape(GROUP_SIZE, ROWS_DEV, IN_WIDTH)
    user_half = lax.map(lambda rows_in: tower_forward(rows_in, user_w1, user_w2, user_w3)[5], user_shards).astype(jnp.bfloat16)
    item_half = lax.map(lambda rows_in: tower_forward(rows_in, item_w1, item_w2, item_w3)[5], item_shards).astype(jnp.bfloat16)
    item_all = item_half.reshape(BATCH, EMBED_DIM)
    cand_pos = jnp.arange(BATCH)

    def query_step(grad_item_sum, shard):
        user_rows, item_rows, id_rows, logq_rows, shard_index = shard
        query_pos = shard_index * ROWS_DEV + jnp.arange(ROWS_DEV)
        raw = jnp.dot(user_rows, item_all.T, preferred_element_type=jnp.float32) * INV_TEMP - log_q[None, :]
        is_self = query_pos[:, None] == cand_pos[None, :]
        dropped = jnp.logical_and(id_rows[:, None] == item_id[None, :], jnp.logical_not(is_self))
        scores = jnp.where(dropped, -jnp.inf, raw)
        row_max = jnp.max(scores, axis=1, keepdims=True)
        exp_scores = jnp.exp(scores - row_max)
        row_total = jnp.sum(exp_scores, axis=1, keepdims=True)
        log_norm = row_max[:, 0] + jnp.log(row_total[:, 0])
        pos_score = jnp.sum(user_rows.astype(jnp.float32) * item_rows.astype(jnp.float32), axis=1) * INV_TEMP - logq_rows
        softmax_rows = exp_scores / row_total
        grad_scores = (jnp.where(is_self, softmax_rows - 1.0, softmax_rows) / BATCH).astype(jnp.bfloat16)
        grad_user = jnp.dot(grad_scores, item_all, preferred_element_type=jnp.float32) * INV_TEMP
        item_part = jnp.dot(grad_scores.T, user_rows, preferred_element_type=jnp.float32) * INV_TEMP
        return grad_item_sum + item_part, (jnp.sum(log_norm - pos_score), grad_user)

    grad_item, step_out = lax.scan(query_step, jnp.zeros((BATCH, EMBED_DIM), jnp.float32),
                                   (user_half, item_half, item_id.reshape(GROUP_SIZE, ROWS_DEV),
                                    log_q.reshape(GROUP_SIZE, ROWS_DEV), jnp.arange(GROUP_SIZE)))
    loss_parts, grad_user = step_out
    user_grads = accumulate_grads(user_shards, grad_user, user_w1, user_w2, user_w3)
    item_grads = accumulate_grads(item_shards, grad_item.reshape(GROUP_SIZE, ROWS_DEV, EMBED_DIM), item_w1, item_w2, item_w3)
    loss = jnp.sum(loss_parts) / BATCH
    return (loss, user_grads[0], user_grads[1], user_grads[2], item_grads[0], item_grads[1], item_grads[2])
```

```python
import jax
import jax.numpy as jnp
from jax import lax
from jax.experimental import pallas as pl
from jax.experimental.pallas import tpu as pltpu
from jax.sharding import PartitionSpec as P

SCALE = 20.0
EPS = 1e-6
NDEV = 16
R = 512
D = 384
H = 1536
B = R * NDEV
BLK = 216
HALF = 8 * BLK
PACK = 2 * HALF
WROWS = 3 * PACK
L = 128
CH = 64
F32, BF16 = jnp.float32, jnp.bfloat16
MESH = pl.DeviceIdType.MESH
NT = (((1,), (1,)), ((), ()))
TN = (((0,), (0,)), ((), ()))
LOWEST = float(jnp.finfo(jnp.float32).min)
V_AG, U_AG = 0, 29
IDS, LQS, STS = 58, 74, 90
AR = (106, 162)
N_SEM = 218
DIMS = (4, 2, 1)


def dot(a, b, dims=(((1,), (0,)), ((), ()))):
    return lax.dot_general(a, b, dims, preferred_element_type=F32)


def kernel(ux, ix, ids_in, lq_in, uw1, uw2, uw3, iw1, iw2, iw3,
           loss, gu1, gu2, gu3, gi1, gi2, gi3,
           S, v_all, u_all, xf, xb, h1, h2, e_ref, inv_ref, w1b, w2b, w3b, da1,
           ids_all, lq_all, st_all, idcol, lqcol, m_ref, l_ref, pos_ref, G, acc, big,
           recv_d, rb1, rb2, rb3, send_sem, recv_sem, loc_sem, out_sem):
    me = lax.axis_index('dp')
    core = lax.rem(me, 2)
    chip = lax.div(me, 2)
    partner = me + 1 - 2 * core

    def flip(m):
        out = 0
        for d in DIMS:
            bit = lax.rem(lax.div(chip, d), 2)
            if isinstance(m, int):
                f = (m // d) % 2
            else:
                f = lax.rem(lax.div(m, d), 2)
            out = out + d * (bit + f - 2 * bit * f)
        return out

    chips = [flip(m) for m in range(8)]

    def nbr(d):
        return chips[d] * 2 + core

    def rc(src, dst, idx, dev):
        return pltpu.make_async_remote_copy(src, dst, send_sem.at[idx], recv_sem.at[idx],
                                            device_id=(dev,), device_id_type=MESH)

    started = []

    def send(src, dst, idx, dev):
        c = rc(src, dst, idx, dev)
        c.start()
        started.append(c)

    def flush():
        for c in started:
            c.wait_send()
        started.clear()

    def arrived(ref, idx):
        rc(ref, ref, idx, partner).wait_recv()

    barrier = pltpu.get_barrier_semaphore()
    for i in range(1, NDEV):
        pl.semaphore_signal(barrier, inc=1, device_id=(lax.rem(me + i, NDEV),), device_id_type=MESH)

    loads = {0: [], 1: []}

    def load(t, src, dst, k):
        c = pltpu.make_async_copy(src, dst, loc_sem.at[t, k])
        c.start()
        loads[t].append(c)

    for t, (xr, w1, w2, w3) in enumerate(((ix, iw1, iw2, iw3), (ux, uw1, uw2, uw3))):
        o = t * WROWS
        load(t, xr, xf.at[t], 0)
        for c in range(12):
            load(t, w1.at[:, pl.ds(L * c, L)], S.at[pl.ds(o + D * c, D), :], 1 + c)
        for c in range(3):
            load(t, w2.at[:, pl.ds(L * c, L)], S.at[pl.ds(o + 4608 + H * c, H), :], 13 + c)
        for c in range(3):
            load(t, w3.at[:, pl.ds(L * c, L)], S.at[pl.ds(o + 9216 + D * c, D), :], 16 + c)

    ids_all[me] = ids_in[...]
    lq_all[me] = lq_in[...]
    idcol[...] = jnp.broadcast_to(ids_in[0:1, :], (L, R)).T
    lqcol[...] = jnp.broadcast_to(lq_in[0:1, :], (L, R)).T

    def forward(t, dest):
        for c in loads[t]:
            c.wait()
        o = t * WROWS
        xb[t] = xf[t].astype(BF16)
        for c in range(12):
            w1b[t, :, L * c:L * c + L] = S[o + D * c:o + D * (c + 1), :].astype(BF16)
        for c in range(3):
            w2b[t, :, L * c:L * c + L] = S[o + 4608 + H * c:o + 4608 + H * (c + 1), :].astype(BF16)
        for c in range(3):
            w3b[t, :, L * c:L * c + L] = S[o + 9216 + D * c:o + 9216 + D * (c + 1), :].astype(BF16)

        def first(n, _):
            cols = pl.ds(pl.multiple_of(n * 256, 256), 256)
            h1[t, :, cols] = jnp.maximum(dot(xb[t], w1b[t, :, cols]), 0.0).astype(BF16)
            return 0
        lax.fori_loop(0, 6, first, 0)
        h2[t] = jnp.maximum(dot(h1[t], w2b[t]), 0.0).astype(BF16)
        z = dot(h2[t], w3b[t])
        inv = lax.rsqrt(jnp.sum(z * z, axis=1, keepdims=True) + EPS)
        inv_ref[t] = jnp.broadcast_to(inv, (R, L))
        e = z * inv
        e_ref[t] = e
        dest[pl.ds(pl.multiple_of(me * R, R), R), :] = e.astype(BF16)

    class Gather:
        def __init__(self, base, part, full):
            self.base, self.part, self.full = base, part, full

        def _send(self, j, pos, rel):
            for p in range(3):
                o = [DIMS[(p + i) % 3] for i in range(3)]
                m = sum(o[i] for i in rel)
                r = self.part(p, chips[m])
                send(r, r, self.base + 7 * p + j, nbr(o[pos]))

        def _wait(self, j, rel):
            for p in range(3):
                o = [DIMS[(p + i) % 3] for i in range(3)]
                m = sum(o[i] for i in rel)
                arrived(self.part(p, chips[m]), self.base + 7 * p + j)

        def _cross(self, m):
            r = self.full(chips[m], core)
            send(r, r, self.base + 21 + m, partner)

        def start(self):
            self._send(0, 0, ())
            self._send(1, 1, ())
            self._send(3, 2, ())
            self._cross(0)

        def f1(self):
            self._wait(0, (0,))
            self._send(2, 1, (0,))
            self._send(4, 2, (0,))

        def f2(self):
            self._wait(1, (1,))
            self._send(5, 2, (1,))

        def f2b(self):
            self._wait(3, (2,))
            for m in (4, 2, 1):
                self._cross(m)

        def f3(self):
            self._wait(2, (0, 1))
            self._send(6, 2, (0, 1))

        def f4(self):
            self._wait(4, (0, 2))
            self._wait(5, (1, 2))
            for m in (6, 5, 3):
                self._cross(m)

        def f5(self):
            self._wait(6, (0, 1, 2))
            self._cross(7)

        def other(self, *ms):
            for m in ms:
                arrived(self.full(chips[m], 1 - core), self.base + 21 + m)

    def emb_gather(buf, base):
        def rows(c, k):
            return pl.ds(pl.multiple_of((c * 2 + k) * R, R), R)
        return Gather(base, lambda p, c: buf.at[rows(c, core), pl.ds(L * p, L)],
                      lambda c, k: buf.at[rows(c, k), :])

    gv = emb_gather(v_all, V_AG)
    gu = emb_gather(u_all, U_AG)

    def wrow(t, p, r):
        return t * WROWS + p * PACK + r

    def wblk(t, p, c, k):
        return pl.ds(pl.multiple_of(wrow(t, p, 0) + (k * 8 + c) * BLK, 8), BLK)

    def add_into(dst_rows, src):
        S[dst_rows, :] += src

    class Reduce:
        def __init__(self, t):
            self.t, self.base = t, AR[t]

        def cross(self):
            for p in range(3):
                rows = pl.ds(pl.multiple_of(wrow(self.t, p, 0) + (1 - core) * HALF, 8), HALF)
                send(S.at[rows, :], recv_d.at[self.t, p], self.base + p, partner)

        def _orders(self):
            for p in range(3):
                yield p, [DIMS[(p + i) % 3] for i in range(3)]

        def p1(self):
            t = self.t
            for p in range(3):
                arrived(recv_d.at[t, p], self.base + p)
            for p in range(3):
                for q in range(8):
                    rows = pl.ds(pl.multiple_of(wrow(t, p, 0) + core * HALF + q * BLK, 8), BLK)
                    S[rows, :] += recv_d[t, p, q * BLK:(q + 1) * BLK, :]
            for s in range(4):
                for p, (a, b, c) in self._orders():
                    m = (b + c, b, c, 0)[s]
                    send(S.at[wblk(t, p, chips[a ^ m], core), :], rb1.at[t, p, s],
                         self.base + 3 + 7 * p + s, nbr(a))

        def p2(self):
            t = self.t
            for s in range(2):
                for p, (a, b, c) in self._orders():
                    m = (b + c, b)[s]
                    arrived(rb1.at[t, p, s], self.base + 3 + 7 * p + s)
                    add_into(wblk(t, p, chips[m], core), rb1[t, p, s])
                    send(S.at[wblk(t, p, chips[m], core), :], rb2.at[t, p, s],
                         self.base + 3 + 7 * p + 4 + s, nbr(b))

        def p2b(self):
            t = self.t
            for s in (2, 3):
                for p, (a, b, c) in self._orders():
                    m = (b + c, b, c, 0)[s]
                    arrived(rb1.at[t, p, s], self.base + 3 + 7 * p + s)
                    add_into(wblk(t, p, chips[m], core), rb1[t, p, s])

        def p3(self):
            t = self.t
            for p, (a, b, c) in self._orders():
                arrived(rb2.at[t, p, 0], self.base + 3 + 7 * p + 4)
                add_into(wblk(t, p, chips[c], core), rb2[t, p, 0])
                send(S.at[wblk(t, p, chips[c], core), :], rb3.at[t, p],
                     self.base + 3 + 7 * p + 6, nbr(c))
            for p, (a, b, c) in self._orders():
                arrived(rb2.at[t, p, 1], self.base + 3 + 7 * p + 5)
                add_into(wblk(t, p, chips[0], core), rb2[t, p, 1])

        def p4(self):
            t = self.t
            for p, (a, b, c) in self._orders():
                arrived(rb3.at[t, p], self.base + 3 + 7 * p + 6)
                S[wblk(t + 1, p, chips[0], core), :] = S[wblk(t, p, chips[0], core), :] + rb3[t, p]

    class GradGather(Gather):
        def __init__(self, t):
            super().__init__(AR[t] + 24, lambda p, c: S.at[wblk(t + 1, p, c, core), :], None)
            self.t = t

        def _cross(self, m):
            for p in range(3):
                r = S.at[wblk(self.t + 1, p, chips[m], core), :]
                send(r, r, N_SEM + self.t * 24 + m * 3 + p, partner)

        def other(self, *ms):
            for m in ms:
                for p in range(3):
                    arrived(S.at[wblk(self.t + 1, p, chips[m], 1 - core), :], N_SEM + self.t * 24 + m * 3 + p)

    def push_all(buf, base):
        for i in range(1, NDEV):
            send(buf.at[me], buf.at[me], base + i, lax.rem(me + i, NDEV))

    def pull_all(buf, base):
        for i in range(1, NDEV):
            arrived(buf.at[lax.rem(me + NDEV - i, NDEV)], base + i)

    def order(i):
        return 4 - 2 * i + lax.div(i * (i - 1), 2)

    def device_of(slot):
        g = lax.div(slot + 1, 3)
        i = lax.rem(slot + 1, 3)
        near = order(i)
        m = jnp.where(slot < 2, 0, jnp.where(g < 3, near, jnp.where(g < 5, 7 - near, 7)))
        oth = jnp.where(slot < 2, slot, jnp.where(slot < 14, lax.rem(g - 1, 2), slot - 14))
        k = core + oth - 2 * core * oth
        return flip(m) * 2 + k

    def rowsl(q):
        return pl.ds(pl.multiple_of(q * R, R), R)

    def diag(r0, t):
        return (lax.broadcasted_iota(jnp.int32, (CH, L), 0) + r0
                == lax.broadcasted_iota(jnp.int32, (CH, L), 1) + L * t)

    def row_slot(slot, own):
        q = me if own else device_of(slot)
        s512 = dot(u_all[rowsl(me), :], v_all[rowsl(q), :], NT)
        for t in range(4):
            S[pl.ds(pl.multiple_of((slot * 4 + t) * R, R), R), :] = s512[:, L * t:L * t + L]

        def chunk(r, _):
            r0 = pl.multiple_of(r * CH, CH)
            rs = pl.ds(r0, CH)
            idc = idcol[rs, :]
            mo = m_ref[rs, :]
            vals = []
            pos = jnp.zeros((CH, L), F32)
            for t in range(4):
                off = pl.ds(pl.multiple_of((slot * 4 + t) * R + r0, CH), CH)
                s = S[off, :] * SCALE - lq_all[q, 0:1, L * t:L * t + L]
                hit = idc == ids_all[q, 0:1, L * t:L * t + L]
                if own:
                    dg = diag(r0, t)
                    pos = pos + jnp.where(dg, s, 0.0)
                    hit = jnp.logical_and(hit, jnp.logical_not(dg))
                s = jnp.where(hit, -jnp.inf, s)
                S[off, :] = s
                vals.append(s)
            if own:
                pos_ref[rs, :] = pos
            mn = jnp.maximum(jnp.maximum(mo, jnp.maximum(vals[0], vals[1])), jnp.maximum(vals[2], vals[3]))
            tot = l_ref[rs, :] * jnp.exp(mo - mn)
            for s in vals:
                tot = tot + jnp.exp(s - mn)
            l_ref[rs, :] = tot
            m_ref[rs, :] = mn
            return 0
        lax.fori_loop(0, R // CH, chunk, 0)

    def row_slots(a, b):
        lax.fori_loop(a, b, lambda s, c: (row_slot(s, False), c)[1], 0)

    def row_finish():
        m = m_ref[...]
        top = jnp.max(m, axis=1, keepdims=True)
        tot = jnp.sum(l_ref[...] * jnp.exp(m - top), axis=1, keepdims=True)
        inv = 1.0 / (tot * float(B))
        cost = top + jnp.log(tot) - jnp.sum(pos_ref[...], axis=1, keepdims=True)
        m_ref[...] = jnp.broadcast_to(top, (R, L))
        l_ref[...] = jnp.broadcast_to(inv, (R, L))
        lane = lax.broadcasted_iota(jnp.int32, (R, L), 1)
        pack = jnp.where(lane == 0, top, jnp.where(lane == 1, inv, jnp.where(lane == 2, cost, 0.0)))
        st_all[me] = pack.T[0:8, :]

    def du_slot(slot, own):
        q = me if own else device_of(slot)

        def chunk(r, _):
            r0 = pl.multiple_of(r * CH, CH)
            rs = pl.ds(r0, CH)
            mc = m_ref[rs, :]
            ic = l_ref[rs, :]
            for t in range(4):
                off = pl.ds(pl.multiple_of((slot * 4 + t) * R + r0, CH), CH)
                g = jnp.exp(S[off, :] - mc) * ic
                if own:
                    g = g - jnp.where(diag(r0, t), 1.0 / B, 0.0)
                G[rs, L * t:L * t + L] = g.astype(BF16)
            return 0
        lax.fori_loop(0, R // CH, chunk, 0)
        part = dot(G[...], v_all[rowsl(q), :])
        acc[...] = part if own else acc[...] + part

    def du_slots(a, b):
        lax.fori_loop(a, b, lambda s, c: (du_slot(s, False), c)[1], 0)

    def dv_slot(slot, own):
        q = me if own else device_of(slot)
        big[...] = dot(v_all[rowsl(me), :], u_all[rowsl(q), :], NT)

        def chunk(r, _):
            r0 = pl.multiple_of(r * CH, CH)
            rs = pl.ds(r0, CH)
            idc = idcol[rs, :]
            lqc = lqcol[rs, :]
            for t in range(4):
                cs = slice(L * t, L * t + L)
                s = big[rs, cs] * SCALE - lqc
                hit = idc == ids_all[q, 0:1, cs]
                if own:
                    dg = diag(r0, t)
                    hit = jnp.logical_and(hit, jnp.logical_not(dg))
                g = jnp.exp(jnp.where(hit, -jnp.inf, s) - st_all[q, 0:1, cs]) * st_all[q, 1:2, cs]
                if own:
                    g = g - jnp.where(dg, 1.0 / B, 0.0)
                G[rs, cs] = g.astype(BF16)
            return 0
        lax.fori_loop(0, R // CH, chunk, 0)
        part = dot(G[...], u_all[rowsl(q), :])
        acc[...] = part if own else acc[...] + part

    def dv_slots(a, b):
        lax.fori_loop(a, b, lambda s, c: (dv_slot(s, False), c)[1], 0)

    def put(t, r0, val):
        n = val.shape[0]
        for p in range(3):
            S[pl.ds(pl.multiple_of(wrow(t, p, 0) + r0, 8), n), :] = val[:, L * p:L * p + L]

    def backward(t):
        d = acc[...] * SCALE
        e = e_ref[t]
        inv = inv_ref[t]
        s = jnp.sum(e * d, axis=1, keepdims=True)
        dzb = ((d - e * s) * jnp.concatenate([inv, inv, inv], axis=1)).astype(BF16)
        put(t, H, dot(h2[t], dzb, TN))
        da2 = jnp.where(h2[t] > 0, dot(dzb, w3b[t], NT), 0.0).astype(BF16)
        G[:, 0:D] = da2

        def mid(c, _):
            cols = pl.ds(pl.multiple_of(c * D, L), D)
            g2 = G[:, 0:D]
            put(t, c * D, dot(h1[t, :, cols], g2, TN))
            g1 = dot(g2, w2b[t, cols, :], NT)
            da1[...] = jnp.where(h1[t, :, cols] > 0, g1, 0.0).astype(BF16)
            put(t, H + D + c * D, dot(xb[t], da1[...], TN))
            return 0
        lax.fori_loop(0, 4, mid, 0)

    outs = {0: (gi1, gi2, gi3), 1: (gu1, gu2, gu3)}
    writes = []

    def write_out(t):
        g1, g2, g3 = outs[t]
        k = 0
        for p in range(3):
            pc = pl.ds(L * p, L)
            jobs = [(wrow(t + 1, p, 0), H, g2.at[:, pc]), (wrow(t + 1, p, H), D, g3.at[:, pc])]
            jobs += [(wrow(t + 1, p, H + D + D * c), D, g1.at[:, pl.ds(D * c + L * p, L)]) for c in range(4)]
            for r0, n, dst in jobs:
                c = pltpu.make_async_copy(S.at[pl.ds(r0, n), :], dst, out_sem.at[t, k])
                c.start()
                writes.append(c)
                k += 1

    forward(0, v_all)
    pl.semaphore_wait(barrier, NDEV - 1)
    gv.start()
    push_all(ids_all, IDS)
    push_all(lq_all, LQS)
    forward(1, u_all)
    gv.f1()
    m_ref[...] = jnp.full((R, L), LOWEST, F32)
    l_ref[...] = jnp.zeros((R, L), F32)
    row_slot(0, True)
    pull_all(ids_all, IDS)
    pull_all(lq_all, LQS)
    gv.other(0)
    gv.f2()
    row_slots(1, 2)
    gv.f2b()
    row_slots(2, 5)
    gv.f3()
    gu.start()
    gv.other(4, 2, 1)
    row_slots(5, 8)
    gv.f4()
    row_slots(8, 11)
    gv.f5()
    gv.other(6, 5, 3)
    row_slots(11, 15)
    gv.other(7)
    row_slots(15, 16)
    row_finish()
    push_all(st_all, STS)
    gu.f1()
    gu.f2()
    du_slot(0, True)
    du_slots(1, 4)
    gu.f2b()
    gu.f3()
    du_slots(4, 12)
    gu.f4()
    du_slots(12, 16)
    gu.f5()
    backward(1)
    ru, ri = Reduce(1), Reduce(0)
    au, ai = GradGather(1), GradGather(0)
    ru.cross()
    pull_all(st_all, STS)
    gu.other(0, 1, 2, 3, 4, 5, 6, 7)
    dv_slot(0, True)
    dv_slots(1, 3)
    ru.p1()
    dv_slots(3, 7)
    ru.p2()
    dv_slots(7, 11)
    ru.p2b()
    dv_slots(11, 14)
    ru.p3()
    dv_slots(14, 16)
    backward(0)
    ru.p4()
    flush()
    au.start()
    ri.cross()
    au.f1()
    au.f2()
    ri.p1()
    au.f2b()
    au.f3()
    au.f4()
    au.f5()
    ri.p2()
    ri.p2b()
    au.other(0, 1, 2, 3, 4, 5, 6, 7)
    write_out(1)
    ri.p3()
    ri.p4()
    ai.start()
    total = jnp.sum(jnp.sum(st_all[...], axis=0)[2:3, :]) * (1.0 / B)
    loss[...] = jnp.full((8, L), total, F32)
    ai.f1()
    ai.f2()
    ai.f2b()
    ai.f3()
    ai.f4()
    ai.f5()
    ai.other(0, 1, 2, 3, 4, 5, 6, 7)
    write_out(0)
    flush()
    for c in writes:
        c.wait()


def solution(mesh):
    vm = pl.BlockSpec(memory_space=pltpu.VMEM)
    hbm = pl.BlockSpec(memory_space=pl.ANY)
    shp = jax.ShapeDtypeStruct
    n_sem = N_SEM + 48

    def device_step(user_x, item_x, item_id, log_q, user_w1, user_w2, user_w3, item_w1, item_w2, item_w3):
        ids8 = jnp.broadcast_to(item_id[None, :], (8, R))
        lq8 = jnp.broadcast_to(log_q[None, :], (8, R))
        V = pltpu.VMEM
        out = pl.pallas_call(
            kernel,
            out_shape=(shp((8, L), F32), shp((D, H), F32), shp((H, D), F32), shp((D, D), F32),
                       shp((D, H), F32), shp((H, D), F32), shp((D, D), F32)),
            in_specs=[hbm, hbm, vm, vm] + [hbm] * 6,
            out_specs=(vm,) + (hbm,) * 6,
            scratch_shapes=[
                V((64 * R, L), F32), V((B, D), BF16), V((B, D), BF16),
                V((2, R, D), F32), V((2, R, D), BF16), V((2, R, H), BF16), V((2, R, D), BF16),
                V((2, R, D), F32), V((2, R, L), F32),
                V((2, D, H), BF16), V((2, H, D), BF16), V((2, D, D), BF16), V((R, D), BF16),
                V((NDEV, 8, R), jnp.int32), V((NDEV, 8, R), F32), V((NDEV, 8, R), F32),
                V((R, L), jnp.int32), V((R, L), F32), V((R, L), F32), V((R, L), F32), V((R, L), F32),
                V((R, R), BF16), V((R, D), F32), V((R, R), F32),
                V((2, 3, HALF, L), F32), V((2, 3, 4, BLK, L), F32), V((2, 3, 2, BLK, L), F32),
                V((2, 3, BLK, L), F32),
                pltpu.SemaphoreType.DMA((n_sem,)), pltpu.SemaphoreType.DMA((n_sem,)),
                pltpu.SemaphoreType.DMA((2, 19)), pltpu.SemaphoreType.DMA((2, 18)),
            ],
            compiler_params=pltpu.CompilerParams(collective_id=0, has_side_effects=True,
                                                 vmem_limit_bytes=67043328),
            name='step',
        )(user_x, item_x, ids8, lq8, user_w1, user_w2, user_w3, item_w1, item_w2, item_w3)
        return (out[0][0, 0],) + tuple(out[1:])

    batch_spec = P('dp', None)
    vec_spec = P('dp')
    whole = P()
    return jax.shard_map(device_step, mesh=mesh,
                         in_specs=(batch_spec, batch_spec, vec_spec, vec_spec, whole, whole, whole, whole, whole, whole),
                         out_specs=(whole,) * 7, check_vma=False)
```

```python
import jax
import jax.numpy as jnp
from jax import lax
from jax.experimental import pallas as pl
from jax.experimental.pallas import tpu as pltpu
from jax.sharding import PartitionSpec as P

SCALE = 20.0
EPS = 1e-6
NDEV = 16
R = 512
D = 384
H = 1536
B = R * NDEV
BLK = 216
HALF = 8 * BLK
PACK = 2 * HALF
SEG = 960
WROWS = 3 * PACK
L = 128
CH = 64
VMEM_LIMIT = 56000000
F32, BF16 = jnp.float32, jnp.bfloat16
MESH = pl.DeviceIdType.MESH
NT = (((1,), (1,)), ((), ()))
TN = (((0,), (0,)), ((), ()))
LOWEST = float(jnp.finfo(jnp.float32).min)
V_AG, U_AG = 0, 29
IDS, LQS, STS = 58, 74, 90
AR = (106, 154)
N_SEM = 202
DIMS = (4, 2, 1)


def dot(a, b, dims=(((1,), (0,)), ((), ()))):
    return lax.dot_general(a, b, dims, preferred_element_type=F32)


def kernel(ux, ix, ids_in, lq_in, uw1, uw2, uw3, iw1, iw2, iw3,
           loss, grads,
           S, v_all, u_all, xb, h1, h2, e_ref, inv_ref, w1b, w2b, w3b, da1,
           ids_all, lq_all, st_all, idcol, lqcol, m_ref, l_ref, pos_ref, G, acc, big,
           recv_d, rb1, rb2, rb3, send_sem, recv_sem, loc_sem, ack):
    me = lax.axis_index('dp')
    core = lax.rem(me, 2)
    chip = lax.div(me, 2)
    partner = me + 1 - 2 * core

    def flip(m):
        out = 0
        for d in DIMS:
            bit = lax.rem(lax.div(chip, d), 2)
            if isinstance(m, int):
                f = (m // d) % 2
            else:
                f = lax.rem(lax.div(m, d), 2)
            out = out + d * (bit + f - 2 * bit * f)
        return out

    chips = [flip(m) for m in range(8)]

    def nbr(d):
        return chips[d] * 2 + core

    def rc(src, dst, idx, dev):
        return pltpu.make_async_remote_copy(src, dst, send_sem.at[idx], recv_sem.at[idx],
                                            device_id=(dev,), device_id_type=MESH)

    started = []

    def send(src, dst, idx, dev):
        c = rc(src, dst, idx, dev)
        c.start()
        started.append(c)

    def flush():
        for c in started:
            c.wait_send()
        started.clear()

    def arrived(ref, idx):
        rc(ref, ref, idx, partner).wait_recv()

    barrier = pltpu.get_barrier_semaphore()
    for i in range(1, NDEV):
        pl.semaphore_signal(barrier, inc=1, device_id=(lax.rem(me + i, NDEV),), device_id_type=MESH)

    loads = {0: [], 1: []}

    def load(t, src, dst, k):
        c = pltpu.make_async_copy(src, dst, loc_sem.at[t, k])
        c.start()
        loads[t].append(c)

    for t, (xr, w1, w2, w3) in enumerate(((ix, iw1, iw2, iw3), (ux, uw1, uw2, uw3))):
        o = t * WROWS
        for c in range(3):
            load(t, xr.at[:, pl.ds(L * c, L)], S.at[pl.ds(2 * WROWS + (3 * t + c) * R, R), :], 19 + c)
        for c in range(12):
            load(t, w1.at[:, pl.ds(L * c, L)], S.at[pl.ds(o + D * c, D), :], 1 + c)
        for c in range(3):
            load(t, w2.at[:, pl.ds(L * c, L)], S.at[pl.ds(o + 4608 + H * c, H), :], 13 + c)
        for c in range(3):
            load(t, w3.at[:, pl.ds(L * c, L)], S.at[pl.ds(o + 9216 + D * c, D), :], 16 + c)

    ids_all[me] = ids_in[...]
    lq_all[me] = lq_in[...]
    for t in range(4):
        idcol[L * t:L * t + L, :] = jnp.broadcast_to(ids_in[t:t + 1, :], (L, L)).T
        lqcol[L * t:L * t + L, :] = jnp.broadcast_to(lq_in[t:t + 1, :], (L, L)).T

    def forward(t, dest):
        for c in loads[t]:
            c.wait()
        o = t * WROWS
        for c in range(3):
            xb[t, :, L * c:L * c + L] = S[2 * WROWS + (3 * t + c) * R:2 * WROWS + (3 * t + c + 1) * R, :].astype(BF16)
        for c in range(12):
            w1b[t, :, L * c:L * c + L] = S[o + D * c:o + D * (c + 1), :].astype(BF16)
        for c in range(3):
            w2b[t, :, L * c:L * c + L] = S[o + 4608 + H * c:o + 4608 + H * (c + 1), :].astype(BF16)
        for c in range(3):
            w3b[t, :, L * c:L * c + L] = S[o + 9216 + D * c:o + 9216 + D * (c + 1), :].astype(BF16)

        def first(n, _):
            cols = pl.ds(pl.multiple_of(n * 256, 256), 256)
            h1[t, :, cols] = jnp.maximum(dot(xb[t], w1b[t, :, cols]), 0.0).astype(BF16)
            return 0
        lax.fori_loop(0, 6, first, 0)
        h2[t] = jnp.maximum(dot(h1[t], w2b[t]), 0.0).astype(BF16)
        z = dot(h2[t], w3b[t])
        inv = lax.rsqrt(jnp.sum(z * z, axis=1, keepdims=True) + EPS)
        inv_ref[t] = jnp.broadcast_to(inv, (R, L))
        e = z * inv
        e_ref[t] = e
        dest[pl.ds(pl.multiple_of(me * R, R), R), :] = e.astype(BF16)

    class Gather:
        def __init__(self, base, part, full):
            self.base, self.part, self.full = base, part, full

        def _send(self, j, pos, rel):
            for p in range(3):
                o = [DIMS[(p + i) % 3] for i in range(3)]
                m = sum(o[i] for i in rel)
                r = self.part(p, chips[m])
                send(r, r, self.base + 7 * p + j, nbr(o[pos]))

        def _wait(self, j, rel):
            for p in range(3):
                o = [DIMS[(p + i) % 3] for i in range(3)]
                m = sum(o[i] for i in rel)
                arrived(self.part(p, chips[m]), self.base + 7 * p + j)

        def _cross(self, m):
            r = self.full(chips[m], core)
            send(r, r, self.base + 21 + m, partner)

        def start(self):
            self._send(0, 0, ())
            self._send(1, 1, ())
            self._send(3, 2, ())
            self._cross(0)

        def f1(self):
            self._wait(0, (0,))
            self._send(2, 1, (0,))
            self._send(4, 2, (0,))

        def f2(self):
            self._wait(1, (1,))
            self._send(5, 2, (1,))

        def f2b(self):
            self._wait(3, (2,))
            for m in (4, 2, 1):
                self._cross(m)

        def f3(self):
            self._wait(2, (0, 1))
            self._send(6, 2, (0, 1))

        def f4(self):
            self._wait(4, (0, 2))
            self._wait(5, (1, 2))
            for m in (6, 5, 3):
                self._cross(m)

        def f5(self):
            self._wait(6, (0, 1, 2))
            self._cross(7)

        def other(self, *ms):
            for m in ms:
                arrived(self.full(chips[m], 1 - core), self.base + 21 + m)

    def emb_gather(buf, base):
        def rows(c, k):
            return pl.ds(pl.multiple_of((c * 2 + k) * R, R), R)
        return Gather(base, lambda p, c: buf.at[rows(c, core), pl.ds(L * p, L)],
                      lambda c, k: buf.at[rows(c, k), :])

    gv = emb_gather(v_all, V_AG)
    gu = emb_gather(u_all, U_AG)

    def wrow(t, p, r):
        return t * WROWS + p * PACK + r

    def wblk(t, p, c, k):
        return pl.ds(pl.multiple_of(wrow(t, p, 0) + (k * 8 + c) * BLK, 8), BLK)

    def add_into(dst_rows, src):
        S[dst_rows, :] += src

    class Reduce:
        def __init__(self, t):
            self.t, self.base = t, AR[t]

        def _segment(self, i):
            o, n = ((0, SEG), (SEG, HALF - SEG))[i]
            for p in range(3):
                rows = pl.ds(pl.multiple_of(wrow(self.t, p, 0) + (1 - core) * HALF + o, 8), n)
                yield S.at[rows, :], recv_d.at[p, pl.ds(o, n), :], self.base + 2 * p + i

        def cross(self, i):
            for src, dst, k in self._segment(i):
                send(src, dst, k, partner)

        def _orders(self):
            for p in range(3):
                yield p, [DIMS[(p + i) % 3] for i in range(3)]

        def p1(self):
            t = self.t
            for i in range(2):
                for src, dst, k in self._segment(i):
                    arrived(dst, k)
            for p in range(3):
                for q in range(8):
                    rows = pl.ds(pl.multiple_of(wrow(t, p, 0) + core * HALF + q * BLK, 8), BLK)
                    S[rows, :] += recv_d[p, q * BLK:(q + 1) * BLK, :]
            if t == 1:
                pl.semaphore_signal(ack, inc=1, device_id=(partner,), device_id_type=MESH)
            for s in range(4):
                for p, (a, b, c) in self._orders():
                    m = (b + c, b, c, 0)[s]
                    send(S.at[wblk(t, p, chips[a ^ m], core), :], rb1.at[p, s],
                         self.base + 6 + 7 * p + s, nbr(a))

        def p2(self):
            t = self.t
            for s in range(2):
                for p, (a, b, c) in self._orders():
                    m = (b + c, b)[s]
                    arrived(rb1.at[p, s], self.base + 6 + 7 * p + s)
                    add_into(wblk(t, p, chips[m], core), rb1[p, s])
                    send(S.at[wblk(t, p, chips[m], core), :], rb2.at[p, s],
                         self.base + 6 + 7 * p + 4 + s, nbr(b))

        def p2b(self):
            t = self.t
            for s in (2, 3):
                for p, (a, b, c) in self._orders():
                    m = (b + c, b, c, 0)[s]
                    arrived(rb1.at[p, s], self.base + 6 + 7 * p + s)
                    add_into(wblk(t, p, chips[m], core), rb1[p, s])

        def p3(self):
            t = self.t
            for p, (a, b, c) in self._orders():
                arrived(rb2.at[p, 0], self.base + 6 + 7 * p + 4)
                add_into(wblk(t, p, chips[c], core), rb2[p, 0])
                send(S.at[wblk(t, p, chips[c], core), :], rb3.at[p],
                     self.base + 6 + 7 * p + 6, nbr(c))
            for p, (a, b, c) in self._orders():
                arrived(rb2.at[p, 1], self.base + 6 + 7 * p + 5)
                add_into(wblk(t, p, chips[0], core), rb2[p, 1])

        def p4(self):
            t = self.t
            for p, (a, b, c) in self._orders():
                arrived(rb3.at[p], self.base + 6 + 7 * p + 6)
                grads[wblk(t, p, chips[0], core), :] = S[wblk(t, p, chips[0], core), :] + rb3[p]

    class GradGather(Gather):
        def __init__(self, t):
            super().__init__(AR[t] + 27, lambda p, c: grads.at[wblk(t, p, c, core), :], None)
            self.t = t

        def _cross(self, m):
            for p in range(3):
                r = grads.at[wblk(self.t, p, chips[m], core), :]
                send(r, r, N_SEM + self.t * 24 + m * 3 + p, partner)

        def other(self, *ms):
            for m in ms:
                for p in range(3):
                    arrived(grads.at[wblk(self.t, p, chips[m], 1 - core), :], N_SEM + self.t * 24 + m * 3 + p)

    def push_all(buf, base):
        for i in range(1, NDEV):
            send(buf.at[me], buf.at[me], base + i, lax.rem(me + i, NDEV))

    def pull_all(buf, base):
        for i in range(1, NDEV):
            arrived(buf.at[lax.rem(me + NDEV - i, NDEV)], base + i)

    def order(i):
        return 4 - 2 * i + lax.div(i * (i - 1), 2)

    def device_of(slot):
        g = lax.div(slot + 1, 3)
        i = lax.rem(slot + 1, 3)
        near = order(i)
        m = jnp.where(slot < 2, 0, jnp.where(g < 3, near, jnp.where(g < 5, 7 - near, 7)))
        oth = jnp.where(slot < 2, slot, jnp.where(slot < 14, lax.rem(g - 1, 2), slot - 14))
        k = core + oth - 2 * core * oth
        return flip(m) * 2 + k

    def rowsl(q):
        return pl.ds(pl.multiple_of(q * R, R), R)

    def diag(r0, t):
        return (lax.broadcasted_iota(jnp.int32, (CH, L), 0) + r0
                == lax.broadcasted_iota(jnp.int32, (CH, L), 1) + L * t)

    def row_slot(slot, own):
        q = me if own else device_of(slot)
        s512 = dot(u_all[rowsl(me), :], v_all[rowsl(q), :], NT)
        for t in range(4):
            S[pl.ds(pl.multiple_of((slot * 4 + t) * R, R), R), :] = s512[:, L * t:L * t + L]

        def chunk(r, _):
            r0 = pl.multiple_of(r * CH, CH)
            rs = pl.ds(r0, CH)
            idc = idcol[rs, :]
            mo = m_ref[rs, :]
            vals = []
            pos = jnp.zeros((CH, L), F32)
            for t in range(4):
                off = pl.ds(pl.multiple_of((slot * 4 + t) * R + r0, CH), CH)
                s = S[off, :] * SCALE - lq_all[q, t:t + 1, :]
                hit = idc == ids_all[q, t:t + 1, :]
                if own:
                    dg = diag(r0, t)
                    pos = pos + jnp.where(dg, s, 0.0)
                    hit = jnp.logical_and(hit, jnp.logical_not(dg))
                s = jnp.where(hit, -jnp.inf, s)
                S[off, :] = s
                vals.append(s)
            if own:
                pos_ref[rs, :] = pos
            mn = jnp.maximum(jnp.maximum(mo, jnp.maximum(vals[0], vals[1])), jnp.maximum(vals[2], vals[3]))
            tot = l_ref[rs, :] * jnp.exp(mo - mn)
            for s in vals:
                tot = tot + jnp.exp(s - mn)
            l_ref[rs, :] = tot
            m_ref[rs, :] = mn
            return 0
        lax.fori_loop(0, R // CH, chunk, 0)

    def row_slots(a, b):
        lax.fori_loop(a, b, lambda s, c: (row_slot(s, False), c)[1], 0)

    def row_finish():
        m = m_ref[...]
        top = jnp.max(m, axis=1, keepdims=True)
        tot = jnp.sum(l_ref[...] * jnp.exp(m - top), axis=1, keepdims=True)
        inv = 1.0 / (tot * float(B))
        cost = top + jnp.log(tot) - jnp.sum(pos_ref[...], axis=1, keepdims=True)
        m_ref[...] = jnp.broadcast_to(top, (R, L))
        l_ref[...] = jnp.broadcast_to(inv, (R, L))
        lane = lax.broadcasted_iota(jnp.int32, (R, L), 1)
        pack = jnp.where(lane == 0, top, jnp.where(lane == 1, inv, jnp.where(lane == 2, cost, 0.0)))
        st_all[me] = pack.T[0:8, :]

    def du_slot(slot, own):
        q = me if own else device_of(slot)

        def chunk(r, _):
            r0 = pl.multiple_of(r * CH, CH)
            rs = pl.ds(r0, CH)
            mc = m_ref[rs, :]
            ic = l_ref[rs, :]
            for t in range(4):
                off = pl.ds(pl.multiple_of((slot * 4 + t) * R + r0, CH), CH)
                g = jnp.exp(S[off, :] - mc) * ic
                if own:
                    g = g - jnp.where(diag(r0, t), 1.0 / B, 0.0)
                G[rs, L * t:L * t + L] = g.astype(BF16)
            return 0
        lax.fori_loop(0, R // CH, chunk, 0)
        part = dot(G[...], v_all[rowsl(q), :])
        acc[...] = part if own else acc[...] + part

    def du_slots(a, b):
        lax.fori_loop(a, b, lambda s, c: (du_slot(s, False), c)[1], 0)

    def dv_slot(slot, own):
        q = me if own else device_of(slot)
        big[...] = dot(v_all[rowsl(me), :], u_all[rowsl(q), :], NT)

        def chunk(r, _):
            r0 = pl.multiple_of(r * CH, CH)
            rs = pl.ds(r0, CH)
            idc = idcol[rs, :]
            lqc = lqcol[rs, :]
            for t in range(4):
                cs = slice(L * t, L * t + L)
                s = big[rs, cs] * SCALE - lqc
                hit = idc == ids_all[q, t:t + 1, :]
                if own:
                    dg = diag(r0, t)
                    hit = jnp.logical_and(hit, jnp.logical_not(dg))
                g = jnp.exp(jnp.where(hit, -jnp.inf, s) - st_all[q, 0:1, cs]) * st_all[q, 1:2, cs]
                if own:
                    g = g - jnp.where(dg, 1.0 / B, 0.0)
                G[rs, cs] = g.astype(BF16)
            return 0
        lax.fori_loop(0, R // CH, chunk, 0)
        part = dot(G[...], u_all[rowsl(q), :])
        acc[...] = part if own else acc[...] + part

    def dv_slots(a, b):
        lax.fori_loop(a, b, lambda s, c: (dv_slot(s, False), c)[1], 0)

    def put(t, r0, val):
        n = val.shape[0]
        for p in range(3):
            S[pl.ds(pl.multiple_of(wrow(t, p, 0) + r0, 8), n), :] = val[:, L * p:L * p + L]

    def backward(t, red, hooks):
        d = acc[...] * SCALE
        e = e_ref[t]
        inv = inv_ref[t]
        s = jnp.sum(e * d, axis=1, keepdims=True)
        dzb = ((d - e * s) * jnp.concatenate([inv, inv, inv], axis=1)).astype(BF16)
        g3 = dot(h2[t], dzb, TN)
        put(t, 2 * D, g3[:D // 2])
        put(t, HALF + 2 * D, g3[D // 2:])
        da2 = jnp.where(h2[t] > 0, dot(dzb, w3b[t], NT), 0.0).astype(BF16)
        G[:, 0:D] = da2

        def mid(i):
            c = lax.rem(i + 2 * (1 - core), 4)
            base = lax.div(c, 2) * HALF + lax.rem(c, 2) * SEG
            cols = pl.ds(pl.multiple_of(c * D, L), D)
            g2 = G[:, 0:D]
            put(t, base, dot(h1[t, :, cols], g2, TN))
            g1 = dot(g2, w2b[t, cols, :], NT)
            da1[...] = jnp.where(h1[t, :, cols] > 0, g1, 0.0).astype(BF16)
            put(t, base + D, dot(xb[t], da1[...], TN))

        hooks[0]()
        for i in range(2):
            mid(i)
            red.cross(i)
        hooks[1]()
        lax.fori_loop(2, 4, lambda i, x: (mid(i), x)[1], 0)

    ru, ri = Reduce(1), Reduce(0)
    au, ai = GradGather(1), GradGather(0)

    def nothing():
        pass

    forward(0, v_all)
    pl.semaphore_wait(barrier, NDEV - 1)
    gv.start()
    push_all(ids_all, IDS)
    push_all(lq_all, LQS)
    forward(1, u_all)
    gv.f1()
    m_ref[...] = jnp.full((R, L), LOWEST, F32)
    l_ref[...] = jnp.zeros((R, L), F32)
    row_slot(0, True)
    pull_all(ids_all, IDS)
    pull_all(lq_all, LQS)
    gv.other(0)
    gv.f2()
    row_slots(1, 2)
    gv.f2b()
    row_slots(2, 5)
    gv.f3()
    gu.start()
    gv.other(4, 2, 1)
    row_slots(5, 8)
    gv.f4()
    row_slots(8, 11)
    gv.f5()
    gv.other(6, 5, 3)
    row_slots(11, 15)
    gv.other(7)
    row_slots(15, 16)
    row_finish()
    push_all(st_all, STS)
    gu.f1()
    gu.f2()
    du_slot(0, True)
    du_slots(1, 5)
    gu.f2b()
    du_slots(5, 10)
    gu.f3()
    du_slots(10, 16)
    backward(1, ru, (nothing, gu.f4))
    gu.f5()
    pull_all(st_all, STS)
    dv_slot(0, True)
    gu.other(0, 4, 2, 1, 6, 5, 3)
    dv_slots(1, 3)
    ru.p1()
    gu.other(7)
    dv_slots(3, 7)
    ru.p2()
    dv_slots(7, 11)
    ru.p2b()
    dv_slots(11, 13)
    ru.p3()
    dv_slots(13, 16)

    def turn():
        ru.p4()
        au.start()
        pl.semaphore_wait(ack, 1)

    backward(0, ri, (turn, nothing))
    au.f1()
    au.f2()
    ri.p1()
    au.f2b()
    au.f3()
    ri.p2()
    ri.p2b()
    au.f4()
    ri.p3()
    au.f5()
    ri.p4()
    ai.start()
    au.other(0, 1, 2, 3, 4, 5, 6, 7)
    total = jnp.sum(jnp.sum(st_all[...], axis=0)[2:3, :]) * (1.0 / B)
    loss[0, 0] = total
    ai.f1()
    ai.f2()
    ai.f2b()
    ai.f3()
    ai.f4()
    ai.f5()
    ai.other(0, 1, 2, 3, 4, 5, 6, 7)
    flush()


def write_kernel(loss_in, grads, loss, gu1, gu2, gu3, gi1, gi2, gi3, sem):
    loss[0, 0] = loss_in[0, 0]
    copies = []
    for t, (g1, g2, g3) in enumerate(((gi1, gi2, gi3), (gu1, gu2, gu3))):
        for p in range(3):
            pc = pl.ds(L * p, L)
            for h in range(2):
                o = t * WROWS + p * PACK + h * HALF
                jobs = [(o + 2 * D, g3.at[pl.ds(h * (D // 2), D // 2), pc])]
                for i in range(2):
                    c = 2 * h + i
                    jobs.append((o + i * SEG, g2.at[pl.ds(D * c, D), pc]))
                    jobs.append((o + i * SEG + D, g1.at[:, pl.ds(D * c + L * p, L)]))
                for r0, dst in jobs:
                    src = grads.at[pl.ds(r0, dst.shape[0]), :]
                    c = pltpu.make_async_copy(src, dst, sem.at[len(copies)])
                    c.start()
                    copies.append(c)
    for c in copies:
        c.wait()


def solution(mesh):
    vm = pl.BlockSpec(memory_space=pltpu.VMEM)
    sm = pl.BlockSpec(memory_space=pltpu.SMEM)
    hbm = pl.BlockSpec(memory_space=pl.ANY)
    shp = jax.ShapeDtypeStruct
    n_sem = N_SEM + 48

    def device_step(user_x, item_x, item_id, log_q, user_w1, user_w2, user_w3, item_w1, item_w2, item_w3):
        V = pltpu.VMEM
        loss, grads = pl.pallas_call(
            kernel,
            out_shape=(shp((1, 1), F32), V((2 * WROWS, L), F32)),
            in_specs=[hbm, hbm, vm, vm] + [hbm] * 6,
            out_specs=(sm, vm),
            scratch_shapes=[
                V((64 * R, L), F32), V((B, D), BF16), V((B, D), BF16),
                V((2, R, D), BF16), V((2, R, H), BF16), V((2, R, D), BF16),
                V((2, R, D), F32), V((2, R, L), F32),
                V((2, D, H), BF16), V((2, H, D), BF16), V((2, D, D), BF16), V((R, D), BF16),
                V((NDEV, 4, L), jnp.int32), V((NDEV, 4, L), F32), V((NDEV, 8, R), F32),
                V((R, L), jnp.int32), V((R, L), F32), V((R, L), F32), V((R, L), F32), V((R, L), F32),
                V((R, R), BF16), V((R, D), F32), V((R, R), F32),
                V((3, HALF, L), F32), V((3, 4, BLK, L), F32), V((3, 2, BLK, L), F32),
                V((3, BLK, L), F32),
                pltpu.SemaphoreType.DMA((n_sem,)), pltpu.SemaphoreType.DMA((n_sem,)),
                pltpu.SemaphoreType.DMA((2, 22)), pltpu.SemaphoreType.REGULAR,
            ],
            compiler_params=pltpu.CompilerParams(collective_id=0, has_side_effects=True,
                                                 vmem_limit_bytes=VMEM_LIMIT),
            name='step',
        )(user_x, item_x, item_id.reshape(4, L), log_q.reshape(4, L),
          user_w1, user_w2, user_w3, item_w1, item_w2, item_w3)
        out = pl.pallas_call(
            write_kernel,
            out_shape=(shp((1, 1), F32), shp((D, H), F32), shp((H, D), F32), shp((D, D), F32),
                       shp((D, H), F32), shp((H, D), F32), shp((D, D), F32)),
            in_specs=[sm, vm],
            out_specs=(sm,) + (hbm,) * 6,
            scratch_shapes=[pltpu.SemaphoreType.DMA((60,))],
            compiler_params=pltpu.CompilerParams(vmem_limit_bytes=1 << 20),
            name='write',
        )(loss, grads)
        return (out[0].reshape(()),) + tuple(out[1:])

    batch_spec = P('dp', None)
    vec_spec = P('dp')
    whole = P()
    return jax.shard_map(device_step, mesh=mesh,
                         in_specs=(batch_spec, batch_spec, vec_spec, vec_spec, whole, whole, whole, whole, whole, whole),
                         out_specs=(whole,) * 7, check_vma=False)
```

```python
import jax
import jax.numpy as jnp
from jax import lax
from jax.experimental import pallas as pl
from jax.experimental.pallas import tpu as pltpu
from jax.sharding import PartitionSpec as P

SCALE = 20.0
EPS = 1e-6
NDEV = 16
R = 512
D = 384
H = 1536
B = R * NDEV
BLK = 216
HALF = 8 * BLK
N_SEND, N_RECV = 9, 89
PACK = 2 * HALF
SEG = 960
WROWS = 3 * PACK
L = 128
CH = 64
VMEM_LIMIT = 56000000
F32, BF16 = jnp.float32, jnp.bfloat16
MESH = pl.DeviceIdType.MESH
NT = (((1,), (1,)), ((), ()))
TN = (((0,), (0,)), ((), ()))
LOWEST = float(jnp.finfo(jnp.float32).min)
DIMS = (4, 2, 1)
CROSS = ((0,), (4, 2, 1), (6, 5, 3), (7,))


def dot(a, b, dims=(((1,), (0,)), ((), ()))):
    return lax.dot_general(a, b, dims, preferred_element_type=F32)


def kernel(ux, ix, ids_in, lq_in, uw1, uw2, uw3, iw1, iw2, iw3,
           loss, grads,
           S, v_all, u_all, xb, h1, h2, e_ref, inv_ref, w1b, w2b, w3b, da1,
           ids_all, lq_all, st_all, idcol, lqcol, m_ref, l_ref, pos_ref, G, acc, big,
           recv_d, rb1, rb2, rb3, send_sem, recv_sem, loc_sem, ack):
    made = [0, 0]

    def new_sems(kind, n):
        made[kind] += n
        return made[kind] - n

    me = lax.axis_index('dp')
    core = lax.rem(me, 2)
    chip = lax.div(me, 2)
    partner = me + 1 - 2 * core

    def flip(m):
        out = 0
        for d in DIMS:
            bit = lax.rem(lax.div(chip, d), 2)
            if isinstance(m, int):
                f = (m // d) % 2
            else:
                f = lax.rem(lax.div(m, d), 2)
            out = out + d * (bit + f - 2 * bit * f)
        return out

    chips = [flip(m) for m in range(8)]

    def nbr(d):
        return chips[d] * 2 + core

    def rc(src, dst, ssem, rsem, dev):
        return pltpu.make_async_remote_copy(src, dst, send_sem.at[ssem], recv_sem.at[rsem],
                                            device_id=(dev,), device_id_type=MESH)

    def send(src, dst, ssem, rsem, dev):
        rc(src, dst, ssem, rsem, dev).start()

    def arrived(ref, rsem):
        rc(ref, ref, 0, rsem, partner).wait_recv()

    def sent(ref, ssem):
        rc(ref, ref, ssem, 0, partner).wait_send()

    barrier = pltpu.get_barrier_semaphore()
    for i in range(1, NDEV):
        pl.semaphore_signal(barrier, inc=1, device_id=(lax.rem(me + i, NDEV),), device_id_type=MESH)

    def load(src, dst, t, k):
        pltpu.make_async_copy(src, dst, loc_sem.at[t, k]).start()

    def loaded(t, k, o, n):
        ref = S.at[pl.ds(o, n), :]
        pltpu.make_async_copy(ref, ref, loc_sem.at[t, k]).wait()

    W2_AT, W3_AT, STAGE = 12 * D, 12 * D + 3 * H, WROWS + 3 * R
    for t, (xr, w1, w2, w3) in enumerate(((ix, iw1, iw2, iw3), (ux, uw1, uw2, uw3))):
        o = t * STAGE

        def columns(src, at, rows, c, k):
            load(src.at[:, pl.ds(L * c, L)], S.at[pl.ds(o + at + rows * c, rows), :], t, k)
        for c in range(3):
            columns(xr, WROWS, R, c, 0)
        for c in range(12):
            columns(w1, 0, D, c, 1 + c // 4)
        for c in range(3):
            columns(w2, W2_AT, H, c, 4)
        for c in range(3):
            columns(w3, W3_AT, D, c, 5)

    ids_all[me] = ids_in[...]
    lq_all[me] = lq_in[...]
    for t in range(4):
        idcol[L * t:L * t + L, :] = jnp.broadcast_to(ids_in[t:t + 1, :], (L, L)).T
        lqcol[L * t:L * t + L, :] = jnp.broadcast_to(lq_in[t:t + 1, :], (L, L)).T

    def forward(t, dest):
        o = t * STAGE

        def take(dst, at, rows, c):
            dst[t, :, L * c:L * c + L] = S[o + at + rows * c:o + at + rows * (c + 1), :].astype(BF16)

        loaded(t, 0, o + WROWS, 3 * R)
        for c in range(3):
            take(xb, WROWS, R, c)
        for n in range(3):
            loaded(t, 1 + n, o + 4 * n * D, 4 * D)
            for c in range(4):
                take(w1b, 0, D, 4 * n + c)
            cols = slice(4 * n * L, 4 * (n + 1) * L)
            h1[t, :, cols] = jnp.maximum(dot(xb[t], w1b[t, :, cols]), 0.0).astype(BF16)
        loaded(t, 4, o + W2_AT, 3 * H)
        for c in range(3):
            take(w2b, W2_AT, H, c)
        h2[t] = jnp.maximum(dot(h1[t], w2b[t]), 0.0).astype(BF16)
        loaded(t, 5, o + W3_AT, 3 * D)
        for c in range(3):
            take(w3b, W3_AT, D, c)
        z = dot(h2[t], w3b[t])
        inv = lax.rsqrt(jnp.sum(z * z, axis=1, keepdims=True) + EPS)
        inv_ref[t] = jnp.broadcast_to(inv, (R, L))
        e = z * inv
        e_ref[t] = e
        dest[pl.ds(pl.multiple_of(me * R, R), R), :] = e.astype(BF16)

    class Gather:
        def __init__(self, part, full, units, ssem):
            self.part, self.full, self.units, self.ssem = part, full, units, ssem
            self.rsem = new_sems(1, 7)
            self.other_sem = None

        def _each(self, rel):
            for p in range(3):
                o = [DIMS[(p + i) % 3] for i in range(3)]
                yield p, o, self.part(p, chips[sum(o[i] for i in rel)])

        def _send(self, j, pos, rel):
            for p, o, r in self._each(rel):
                send(r, r, self.ssem, self.rsem + j, nbr(o[pos]))

        def _wait(self, j):
            arrived(self.units(3), self.rsem + j)

        def _cross(self, g):
            if self.other_sem is None:
                self.other_sem = self.cross_sems()
            for m in CROSS[g]:
                for r in self.full(chips[m]):
                    send(r, r, self.ssem, self.other_sem[g], partner)

        def start(self):
            self._send(0, 0, ())
            self._send(1, 1, ())
            self._send(3, 2, ())
            self._cross(0)

        def f1(self):
            self._wait(0)
            self._send(2, 1, (0,))
            self._send(4, 2, (0,))

        def f2(self):
            self._wait(1)
            self._send(5, 2, (1,))

        def f2b(self):
            self._wait(3)
            self._cross(1)

        def f3(self):
            self._wait(2)
            self._send(6, 2, (0, 1))

        def f4(self):
            self._wait(4)
            self._wait(5)
            self._cross(2)

        def f5(self):
            self._wait(6)
            self._cross(3)

    class Embeddings(Gather):
        def __init__(self, buf):
            def rows(c):
                return pl.ds(pl.multiple_of((c * 2 + core) * R, R), R)
            self.buf = buf
            super().__init__(lambda p, c: buf.at[rows(c), pl.ds(L * p, L)], lambda c: (buf.at[rows(c), :],),
                             lambda n: buf.at[pl.ds(0, n // 3 * R), :], new_sems(0, 1))

        def cross_sems(self):
            k = new_sems(1, 4)
            return range(k, k + 4)

        def other(self, g):
            arrived(self.units(3 * len(CROSS[g])), self.other_sem[g])

        def finish(self):
            sent(self.units(3 * (NDEV - 1)), self.ssem)

    gv = Embeddings(v_all)
    gu = Embeddings(u_all)

    def wrow(t, p, r):
        return t * WROWS + p * PACK + r

    class Reduce(Gather):
        def __init__(self, t, piece):
            self.t, self.piece = t, piece
            self.at, self.blk = ((0, SEG // 8), (SEG, (HALF - SEG) // 8))[piece]
            self.sub = (0, SEG // 8)[piece]
            super().__init__(lambda p, c: grads.at[self.rows(p, c), :], self._all_parts,
                             lambda n: grads.at[pl.ds(0, n * self.blk), :], new_sems(0, 1))
            self.red = new_sems(1, 8)

        def rows(self, p, c):
            return pl.ds(pl.multiple_of(wrow(self.t, p, 0) + core * HALF + self.at + c * self.blk, 8), self.blk)

        def _all_parts(self, c):
            return [grads.at[self.rows(p, c), :] for p in range(3)]

        def cross_sems(self):
            return (new_sems(1, 1),) * 4

        def other(self):
            arrived(self.units(24), self.other_sem[0])

        def finish(self):
            sent(self.units(90), self.ssem)

        def cross(self):
            n = 8 * self.blk
            for p in range(3):
                rows = pl.ds(pl.multiple_of(wrow(self.t, p, 0) + (1 - core) * HALF + self.at, 8), n)
                send(S.at[rows, :], recv_d.at[p, pl.ds(self.at, n), :], self.ssem, self.red, partner)

        def _orders(self):
            for p in range(3):
                yield p, [DIMS[(p + i) % 3] for i in range(3)]

        def _got(self, k):
            arrived(self.units(3), self.red + k)

        def _buf(self, ref, *i):
            return ref.at[(*i, pl.ds(self.sub, self.blk), slice(None))]

        def _add(self, p, c, ref, *i):
            rows = self.rows(p, c)
            S[rows, :] += self._buf(ref, *i)[...]

        def _pass(self, p, c, k, dev, ref, *i):
            send(S.at[self.rows(p, c), :], self._buf(ref, *i), self.ssem, self.red + k, nbr(dev))

        def p1(self):
            arrived(self.units(24), self.red)
            for p in range(3):
                for q in range(8):
                    rows = self.rows(p, q)
                    S[rows, :] += recv_d[p, self.at + q * self.blk:self.at + (q + 1) * self.blk, :]
            if self.t == 1:
                pl.semaphore_signal(ack.at[self.piece], inc=1, device_id=(partner,), device_id_type=MESH)
            for s in range(4):
                for p, (a, b, c) in self._orders():
                    self._pass(p, chips[a ^ (b + c, b, c, 0)[s]], 1 + s, a, rb1, p, s)

        def p2(self):
            for s in range(2):
                self._got(1 + s)
                for p, (a, b, c) in self._orders():
                    m = (b + c, b)[s]
                    self._add(p, chips[m], rb1, p, s)
                    self._pass(p, chips[m], 5 + s, b, rb2, p, s)

        def p2b(self):
            for s in (2, 3):
                self._got(1 + s)
                for p, (a, b, c) in self._orders():
                    self._add(p, chips[(c, 0)[s - 2]], rb1, p, s)

        def p3(self):
            self._got(5)
            for p, (a, b, c) in self._orders():
                self._add(p, chips[c], rb2, p, 0)
                self._pass(p, chips[c], 7, c, rb3, p)
            self._got(6)
            for p, (a, b, c) in self._orders():
                self._add(p, chips[0], rb2, p, 1)

        def p4(self):
            self._got(7)
            for p in range(3):
                rows = self.rows(p, chips[0])
                grads[rows, :] = S[rows, :] + self._buf(rb3, p)[...]
            self.start()

    class Push:
        def __init__(self, buf):
            self.buf, self.ssem, self.rsem = buf, new_sems(0, 1), new_sems(1, 1)

        def start(self):
            for i in range(1, NDEV):
                send(self.buf.at[me], self.buf.at[me], self.ssem, self.rsem, lax.rem(me + i, NDEV))

        def wait(self):
            arrived(self.buf.at[pl.ds(0, NDEV - 1)], self.rsem)

        def finish(self):
            sent(self.buf.at[pl.ds(0, NDEV - 1)], self.ssem)

    def order(i):
        return 4 - 2 * i + lax.div(i * (i - 1), 2)

    def device_of(slot):
        g = lax.div(slot + 1, 3)
        i = lax.rem(slot + 1, 3)
        near = order(i)
        m = jnp.where(slot < 2, 0, jnp.where(g < 3, near, jnp.where(g < 5, 7 - near, 7)))
        oth = jnp.where(slot < 2, slot, jnp.where(slot < 14, lax.rem(g - 1, 2), slot - 14))
        k = core + oth - 2 * core * oth
        return flip(m) * 2 + k

    def rowsl(q):
        return pl.ds(pl.multiple_of(q * R, R), R)

    def diag(r0, t):
        return (lax.broadcasted_iota(jnp.int32, (CH, L), 0) + r0
                == lax.broadcasted_iota(jnp.int32, (CH, L), 1) + L * t)

    def row_slot(slot, own):
        q = me if own else device_of(slot)
        s512 = dot(u_all[rowsl(me), :], v_all[rowsl(q), :], NT)
        for t in range(4):
            S[pl.ds(pl.multiple_of((slot * 4 + t) * R, R), R), :] = s512[:, L * t:L * t + L]

        def chunk(r, _):
            r0 = pl.multiple_of(r * CH, CH)
            rs = pl.ds(r0, CH)
            idc = idcol[rs, :]
            mo = m_ref[rs, :]
            vals = []
            pos = jnp.zeros((CH, L), F32)
            for t in range(4):
                off = pl.ds(pl.multiple_of((slot * 4 + t) * R + r0, CH), CH)
                s = S[off, :] * SCALE - lq_all[q, t:t + 1, :]
                hit = idc == ids_all[q, t:t + 1, :]
                if own:
                    dg = diag(r0, t)
                    pos = pos + jnp.where(dg, s, 0.0)
                    hit = jnp.logical_and(hit, jnp.logical_not(dg))
                s = jnp.where(hit, -jnp.inf, s)
                S[off, :] = s
                vals.append(s)
            if own:
                pos_ref[rs, :] = pos
            mn = jnp.maximum(jnp.maximum(mo, jnp.maximum(vals[0], vals[1])), jnp.maximum(vals[2], vals[3]))
            tot = l_ref[rs, :] * jnp.exp(mo - mn)
            for s in vals:
                tot = tot + jnp.exp(s - mn)
            l_ref[rs, :] = tot
            m_ref[rs, :] = mn
            return 0
        lax.fori_loop(0, R // CH, chunk, 0)

    def row_slots(a, b):
        lax.fori_loop(a, b, lambda s, c: (row_slot(s, False), c)[1], 0)

    def row_finish():
        m = m_ref[...]
        top = jnp.max(m, axis=1, keepdims=True)
        tot = jnp.sum(l_ref[...] * jnp.exp(m - top), axis=1, keepdims=True)
        inv = 1.0 / (tot * float(B))
        cost = top + jnp.log(tot) - jnp.sum(pos_ref[...], axis=1, keepdims=True)
        m_ref[...] = jnp.broadcast_to(top, (R, L))
        l_ref[...] = jnp.broadcast_to(inv, (R, L))
        lane = lax.broadcasted_iota(jnp.int32, (R, L), 1)
        pack = jnp.where(lane == 0, top, jnp.where(lane == 1, inv, jnp.where(lane == 2, cost, 0.0)))
        st_all[me] = pack.T[0:8, :]

    def du_slot(slot, own):
        q = me if own else device_of(slot)

        def chunk(r, _):
            r0 = pl.multiple_of(r * CH, CH)
            rs = pl.ds(r0, CH)
            mc = m_ref[rs, :]
            ic = l_ref[rs, :]
            for t in range(4):
                off = pl.ds(pl.multiple_of((slot * 4 + t) * R + r0, CH), CH)
                g = jnp.exp(S[off, :] - mc) * ic
                if own:
                    g = g - jnp.where(diag(r0, t), 1.0 / B, 0.0)
                G[rs, L * t:L * t + L] = g.astype(BF16)
            return 0
        lax.fori_loop(0, R // CH, chunk, 0)
        part = dot(G[...], v_all[rowsl(q), :])
        acc[...] = part if own else acc[...] + part

    def du_slots(a, b):
        lax.fori_loop(a, b, lambda s, c: (du_slot(s, False), c)[1], 0)

    def dv_slot(slot, own):
        q = me if own else device_of(slot)
        big[...] = dot(v_all[rowsl(me), :], u_all[rowsl(q), :], NT)

        def chunk(r, _):
            r0 = pl.multiple_of(r * CH, CH)
            rs = pl.ds(r0, CH)
            idc = idcol[rs, :]
            lqc = lqcol[rs, :]
            for t in range(4):
                cs = slice(L * t, L * t + L)
                s = big[rs, cs] * SCALE - lqc
                hit = idc == ids_all[q, t:t + 1, :]
                if own:
                    dg = diag(r0, t)
                    hit = jnp.logical_and(hit, jnp.logical_not(dg))
                g = jnp.exp(jnp.where(hit, -jnp.inf, s) - st_all[q, 0:1, cs]) * st_all[q, 1:2, cs]
                if own:
                    g = g - jnp.where(dg, 1.0 / B, 0.0)
                G[rs, cs] = g.astype(BF16)
            return 0
        lax.fori_loop(0, R // CH, chunk, 0)
        part = dot(G[...], u_all[rowsl(q), :])
        acc[...] = part if own else acc[...] + part

    def dv_slots(a, b):
        lax.fori_loop(a, b, lambda s, c: (dv_slot(s, False), c)[1], 0)

    def put(t, r0, val):
        n = val.shape[0]
        for p in range(3):
            S[pl.ds(pl.multiple_of(wrow(t, p, 0) + r0, 8), n), :] = val[:, L * p:L * p + L]

    def backward(t, reds, hooks):
        d = acc[...] * SCALE
        e = e_ref[t]
        inv = inv_ref[t]
        s = jnp.sum(e * d, axis=1, keepdims=True)
        dzb = ((d - e * s) * jnp.concatenate([inv, inv, inv], axis=1)).astype(BF16)
        g3 = dot(h2[t], dzb, TN)
        put(t, 2 * D, g3[:D // 2])
        put(t, HALF + 2 * D, g3[D // 2:])
        da2 = jnp.where(h2[t] > 0, dot(dzb, w3b[t], NT), 0.0).astype(BF16)
        G[:, 0:D] = da2

        def mid(i):
            c = lax.rem(i + 2 * (1 - core), 4)
            base = lax.div(c, 2) * HALF + lax.rem(c, 2) * SEG
            cols = pl.ds(pl.multiple_of(c * D, L), D)
            g2 = G[:, 0:D]
            put(t, base, dot(h1[t, :, cols], g2, TN))
            g1 = dot(g2, w2b[t, cols, :], NT)
            da1[...] = jnp.where(h1[t, :, cols] > 0, g1, 0.0).astype(BF16)
            put(t, base + D, dot(xb[t], da1[...], TN))

        hooks[0]()
        mid(0)
        hooks[1]()
        reds[0].cross()
        mid(1)
        hooks[2]()
        reds[1].cross()
        lax.fori_loop(2, 4, lambda i, x: (mid(i), x)[1], 0)

    pi, pq, ps = Push(ids_all), Push(lq_all), Push(st_all)
    ua, ub, ia, ib = Reduce(1, 0), Reduce(1, 1), Reduce(0, 0), Reduce(0, 1)

    def nothing():
        pass

    forward(0, v_all)
    pl.semaphore_wait(barrier, NDEV - 1)
    gv.start()
    pi.start()
    pq.start()
    forward(1, u_all)
    gv.f1()
    m_ref[...] = jnp.full((R, L), LOWEST, F32)
    l_ref[...] = jnp.zeros((R, L), F32)
    row_slot(0, True)
    pi.wait()
    pq.wait()
    gv.other(0)
    gv.f2()
    row_slots(1, 2)
    gv.f2b()
    row_slots(2, 5)
    gv.f3()
    gu.start()
    gv.other(1)
    row_slots(5, 8)
    gv.f4()
    row_slots(8, 11)
    gv.f5()
    gv.other(2)
    row_slots(11, 15)
    gv.other(3)
    row_slots(15, 16)
    row_finish()
    ps.start()
    gu.f1()
    gu.f2()
    du_slot(0, True)
    du_slots(1, 5)
    gu.f2b()
    du_slots(5, 10)
    gu.f3()
    du_slots(10, 16)
    backward(1, (ua, ub), (nothing, gu.f4, nothing))
    gu.f5()
    ua.p1()
    ps.wait()
    dv_slot(0, True)
    ub.p1()
    gu.other(0)
    gu.other(1)
    dv_slots(1, 4)
    ua.p2()
    gu.other(2)
    gu.other(3)
    dv_slots(4, 6)
    ua.p2b()
    dv_slots(6, 8)
    ub.p2()
    dv_slots(8, 10)
    ub.p2b()
    dv_slots(10, 12)
    ua.p3()
    dv_slots(12, 13)
    ub.p3()
    dv_slots(13, 14)
    ua.p4()
    dv_slots(14, 16)
    ub.p4()

    def turn(i):
        def go():
            (ua, ub)[i].f1()
            pl.semaphore_wait(ack.at[i], 1)
        return go

    backward(0, (ia, ib), (nothing, turn(0), turn(1)))
    ua.f2()
    ia.p1()
    ub.f2()
    ib.p1()
    ua.f2b()
    ua.f3()
    ia.p2()
    ub.f2b()
    ub.f3()
    ia.p2b()
    ib.p2()
    ib.p2b()
    ua.f4()
    ia.p3()
    ub.f4()
    ib.p3()
    ia.p4()
    ua.f5()
    ib.p4()
    ub.f5()
    total = jnp.sum(jnp.sum(st_all[...], axis=0)[2:3, :]) * (1.0 / B)
    loss[0, 0] = total
    ia.f1()
    ia.f2()
    ib.f1()
    ib.f2()
    ua.other()
    ub.other()
    ia.f2b()
    ia.f3()
    ib.f2b()
    ib.f3()
    ia.f4()
    ib.f4()
    ia.f5()
    ib.f5()
    ia.other()
    ib.other()
    for x in (gv, gu, pi, pq, ps, ua, ub, ia, ib):
        x.finish()


def write_kernel(loss_in, grads, loss, gu1, gu2, gu3, gi1, gi2, gi3, sem):
    loss[0, 0] = loss_in[0, 0]
    for t, (g1, g2, g3) in enumerate(((gi1, gi2, gi3), (gu1, gu2, gu3))):
        for p in range(3):
            pc = pl.ds(L * p, L)
            for h in range(2):
                o = t * WROWS + p * PACK + h * HALF
                jobs = [(o + 2 * D, g3.at[pl.ds(h * (D // 2), D // 2), pc])]
                for i in range(2):
                    c = 2 * h + i
                    jobs.append((o + i * SEG, g2.at[pl.ds(D * c, D), pc]))
                    jobs.append((o + i * SEG + D, g1.at[:, pl.ds(D * c + L * p, L)]))
                for r0, dst in jobs:
                    src = grads.at[pl.ds(r0, dst.shape[0]), :]
                    pltpu.make_async_copy(src, dst, sem).start()
    pltpu.make_async_copy(grads, grads, sem).wait()


def solution(mesh):
    vm = pl.BlockSpec(memory_space=pltpu.VMEM)
    sm = pl.BlockSpec(memory_space=pltpu.SMEM)
    hbm = pl.BlockSpec(memory_space=pl.ANY)
    shp = jax.ShapeDtypeStruct

    def device_step(user_x, item_x, item_id, log_q, user_w1, user_w2, user_w3, item_w1, item_w2, item_w3):
        V = pltpu.VMEM
        loss, grads = pl.pallas_call(
            kernel,
            out_shape=(shp((1, 1), F32), V((2 * WROWS, L), F32)),
            in_specs=[hbm, hbm, vm, vm] + [hbm] * 6,
            out_specs=(sm, vm),
            scratch_shapes=[
                V((64 * R, L), F32), V((B, D), BF16), V((B, D), BF16),
                V((2, R, D), BF16), V((2, R, H), BF16), V((2, R, D), BF16),
                V((2, R, D), F32), V((2, R, L), F32),
                V((2, D, H), BF16), V((2, H, D), BF16), V((2, D, D), BF16), V((R, D), BF16),
                V((NDEV, 4, L), jnp.int32), V((NDEV, 4, L), F32), V((NDEV, 8, R), F32),
                V((R, L), jnp.int32), V((R, L), F32), V((R, L), F32), V((R, L), F32), V((R, L), F32),
                V((R, R), BF16), V((R, D), F32), V((R, R), F32),
                V((3, HALF, L), F32), V((3, 4, BLK, L), F32), V((3, 2, BLK, L), F32),
                V((3, BLK, L), F32),
                pltpu.SemaphoreType.DMA((N_SEND,)), pltpu.SemaphoreType.DMA((N_RECV,)),
                pltpu.SemaphoreType.DMA((2, 6)), pltpu.SemaphoreType.REGULAR((2,)),
            ],
            compiler_params=pltpu.CompilerParams(collective_id=0, has_side_effects=True,
                                                 vmem_limit_bytes=VMEM_LIMIT),
            name='step',
        )(user_x, item_x, item_id.reshape(4, L), log_q.reshape(4, L),
          user_w1, user_w2, user_w3, item_w1, item_w2, item_w3)
        out = pl.pallas_call(
            write_kernel,
            out_shape=(shp((1, 1), F32), shp((D, H), F32), shp((H, D), F32), shp((D, D), F32),
                       shp((D, H), F32), shp((H, D), F32), shp((D, D), F32)),
            in_specs=[sm, vm],
            out_specs=(sm,) + (hbm,) * 6,
            scratch_shapes=[pltpu.SemaphoreType.DMA],
            compiler_params=pltpu.CompilerParams(vmem_limit_bytes=1 << 20),
            name='write',
        )(loss, grads)
        return (out[0].reshape(()),) + tuple(out[1:])

    batch_spec = P('dp', None)
    vec_spec = P('dp')
    whole = P()
    return jax.shard_map(device_step, mesh=mesh,
                         in_specs=(batch_spec, batch_spec, vec_spec, vec_spec, whole, whole, whole, whole, whole, whole),
                         out_specs=(whole,) * 7, check_vma=False)
```

```python
import jax
import jax.numpy as jnp
from jax import lax
from jax.experimental import pallas as pl
from jax.experimental.pallas import tpu as pltpu
from jax.sharding import PartitionSpec as P

SCALE = 20.0
EPS = 1e-6
NDEV = 16
R = 512
D = 384
H = 1536
B = R * NDEV
BLK = 216
HALF = 8 * BLK
N_SEND, N_RECV = 9, 89
PACK = 2 * HALF
SEG = 960
WROWS = 3 * PACK
L = 128
CH = 64
VMEM_LIMIT = 56000000
F32, BF16 = jnp.float32, jnp.bfloat16
MESH = pl.DeviceIdType.MESH
NT = (((1,), (1,)), ((), ()))
TN = (((0,), (0,)), ((), ()))
LOWEST = float(jnp.finfo(jnp.float32).min)
DIMS = (4, 2, 1)
CROSS = ((0,), (4, 2, 1), (6, 5, 3), (7,))


def dot(a, b, dims=(((1,), (0,)), ((), ()))):
    return lax.dot_general(a, b, dims, preferred_element_type=F32)


def kernel(ux, ix, ids_in, lq_in, uw1, uw2, uw3, iw1, iw2, iw3,
           loss, grads,
           S, v_all, u_all, xb, h1, h2, e_ref, inv_ref, w1b, w2b, w3b, da1,
           ids_all, lq_all, st_all, idcol, lqcol, m_ref, l_ref, pos_ref, G, acc, big,
           recv_d, rb1, rb2, rb3, send_sem, recv_sem, loc_sem, ack):
    made = [0, 0]

    def new_sems(kind, n):
        made[kind] += n
        return made[kind] - n

    me = lax.axis_index('dp')
    core = lax.rem(me, 2)
    chip = lax.div(me, 2)
    partner = me + 1 - 2 * core

    def flip(m):
        out = 0
        for d in DIMS:
            bit = lax.rem(lax.div(chip, d), 2)
            if isinstance(m, int):
                f = (m // d) % 2
            else:
                f = lax.rem(lax.div(m, d), 2)
            out = out + d * (bit + f - 2 * bit * f)
        return out

    chips = [flip(m) for m in range(8)]

    def nbr(d):
        return chips[d] * 2 + core

    def rc(src, dst, ssem, rsem, dev):
        return pltpu.make_async_remote_copy(src, dst, send_sem.at[ssem], recv_sem.at[rsem],
                                            device_id=(dev,), device_id_type=MESH)

    def send(src, dst, ssem, rsem, dev):
        rc(src, dst, ssem, rsem, dev).start()

    def arrived(ref, rsem):
        rc(ref, ref, 0, rsem, partner).wait_recv()

    def sent(ref, ssem):
        rc(ref, ref, ssem, 0, partner).wait_send()

    barrier = pltpu.get_barrier_semaphore()
    for i in range(1, NDEV):
        pl.semaphore_signal(barrier, inc=1, device_id=(lax.rem(me + i, NDEV),), device_id_type=MESH)

    def load(src, dst, t, k):
        pltpu.make_async_copy(src, dst, loc_sem.at[t, k]).start()

    def loaded(t, k, o, n):
        ref = S.at[pl.ds(o, n), :]
        pltpu.make_async_copy(ref, ref, loc_sem.at[t, k]).wait()

    W2_AT, W3_AT, STAGE = 12 * D, 12 * D + 3 * H, WROWS + 3 * R
    for t, (xr, w1, w2, w3) in enumerate(((ix, iw1, iw2, iw3), (ux, uw1, uw2, uw3))):
        o = t * STAGE

        def columns(src, at, rows, c, k):
            load(src.at[:, pl.ds(L * c, L)], S.at[pl.ds(o + at + rows * c, rows), :], t, k)
        for c in range(3):
            columns(xr, WROWS, R, c, 0)
        for c in range(12):
            columns(w1, 0, D, c, 1 + c // 4)
        for c in range(3):
            columns(w2, W2_AT, H, c, 4)
        for c in range(3):
            columns(w3, W3_AT, D, c, 5)

    ids_all[me] = ids_in[...]
    lq_all[me] = lq_in[...]
    for t in range(4):
        idcol[L * t:L * t + L, :] = jnp.broadcast_to(ids_in[t:t + 1, :], (L, L)).T
        lqcol[L * t:L * t + L, :] = jnp.broadcast_to(lq_in[t:t + 1, :], (L, L)).T

    def forward(t, dest):
        o = t * STAGE

        def take(dst, at, rows, c):
            dst[t, :, L * c:L * c + L] = S[o + at + rows * c:o + at + rows * (c + 1), :].astype(BF16)

        loaded(t, 0, o + WROWS, 3 * R)
        for c in range(3):
            take(xb, WROWS, R, c)
        for n in range(3):
            loaded(t, 1 + n, o + 4 * n * D, 4 * D)
            for c in range(4):
                take(w1b, 0, D, 4 * n + c)
            cols = slice(4 * n * L, 4 * (n + 1) * L)
            h1[t, :, cols] = jnp.maximum(dot(xb[t], w1b[t, :, cols]), 0.0).astype(BF16)
        loaded(t, 4, o + W2_AT, 3 * H)
        for c in range(3):
            take(w2b, W2_AT, H, c)
        h2[t] = jnp.maximum(dot(h1[t], w2b[t]), 0.0).astype(BF16)
        loaded(t, 5, o + W3_AT, 3 * D)
        for c in range(3):
            take(w3b, W3_AT, D, c)
        z = dot(h2[t], w3b[t])
        inv = lax.rsqrt(jnp.sum(z * z, axis=1, keepdims=True) + EPS)
        inv_ref[t] = jnp.broadcast_to(inv, (R, L))
        e = z * inv
        e_ref[t] = e
        dest[pl.ds(pl.multiple_of(me * R, R), R), :] = e.astype(BF16)

    class Gather:
        def __init__(self, part, full, units, ssem):
            self.part, self.full, self.units, self.ssem = part, full, units, ssem
            self.rsem = new_sems(1, 7)
            self.other_sem = None

        def _each(self, rel):
            for p in range(3):
                o = [DIMS[(p + i) % 3] for i in range(3)]
                yield p, o, self.part(p, chips[sum(o[i] for i in rel)])

        def _send(self, j, pos, rel):
            for p, o, r in self._each(rel):
                send(r, r, self.ssem, self.rsem + j, nbr(o[pos]))

        def _wait(self, j):
            arrived(self.units(3), self.rsem + j)

        def _cross(self, g):
            if self.other_sem is None:
                self.other_sem = self.cross_sems()
            for m in CROSS[g]:
                for r in self.full(chips[m]):
                    send(r, r, self.ssem, self.other_sem[g], partner)

        def start(self):
            self._send(0, 0, ())
            self._send(1, 1, ())
            self._send(3, 2, ())
            self._cross(0)

        def f1(self):
            self._wait(0)
            self._send(2, 1, (0,))
            self._send(4, 2, (0,))

        def f2(self):
            self._wait(1)
            self._send(5, 2, (1,))

        def f2b(self):
            self._wait(3)
            self._cross(1)

        def f3(self):
            self._wait(2)
            self._send(6, 2, (0, 1))

        def f4(self):
            self._wait(4)
            self._wait(5)
            self._cross(2)

        def f5(self):
            self._wait(6)
            self._cross(3)

    class Embeddings(Gather):
        def __init__(self, buf):
            def rows(c):
                return pl.ds(pl.multiple_of((c * 2 + core) * R, R), R)
            self.buf = buf
            super().__init__(lambda p, c: buf.at[rows(c), pl.ds(L * p, L)], lambda c: (buf.at[rows(c), :],),
                             lambda n: buf.at[pl.ds(0, n // 3 * R), :], new_sems(0, 1))

        def cross_sems(self):
            k = new_sems(1, 4)
            return range(k, k + 4)

        def other(self, g):
            arrived(self.units(3 * len(CROSS[g])), self.other_sem[g])

        def finish(self):
            sent(self.units(3 * (NDEV - 1)), self.ssem)

    gv = Embeddings(v_all)
    gu = Embeddings(u_all)

    def wrow(t, p, r):
        return t * WROWS + p * PACK + r

    class Reduce(Gather):
        def __init__(self, t, piece):
            self.t, self.piece = t, piece
            self.at, self.blk = ((0, SEG // 8), (SEG, (HALF - SEG) // 8))[piece]
            self.sub = (0, SEG // 8)[piece]
            super().__init__(lambda p, c: grads.at[self.rows(p, c), :], self._all_parts,
                             lambda n: grads.at[pl.ds(0, n * self.blk), :], new_sems(0, 1))
            self.red = new_sems(1, 8)

        def rows(self, p, c):
            return pl.ds(pl.multiple_of(wrow(self.t, p, 0) + core * HALF + self.at + c * self.blk, 8), self.blk)

        def _all_parts(self, c):
            return [grads.at[self.rows(p, c), :] for p in range(3)]

        def cross_sems(self):
            return (new_sems(1, 1),) * 4

        def other(self):
            arrived(self.units(24), self.other_sem[0])

        def finish(self):
            sent(self.units(90), self.ssem)

        def cross(self):
            n = 8 * self.blk
            for p in range(3):
                rows = pl.ds(pl.multiple_of(wrow(self.t, p, 0) + (1 - core) * HALF + self.at, 8), n)
                send(S.at[rows, :], recv_d.at[p, pl.ds(self.at, n), :], self.ssem, self.red, partner)

        def _orders(self):
            for p in range(3):
                yield p, [DIMS[(p + i) % 3] for i in range(3)]

        def _got(self, k):
            arrived(self.units(3), self.red + k)

        def _buf(self, ref, *i):
            return ref.at[(*i, pl.ds(self.sub, self.blk), slice(None))]

        def _add(self, p, c, ref, *i):
            rows = self.rows(p, c)
            S[rows, :] += self._buf(ref, *i)[...]

        def _pass(self, p, c, k, dev, ref, *i):
            send(S.at[self.rows(p, c), :], self._buf(ref, *i), self.ssem, self.red + k, nbr(dev))

        def p1(self):
            arrived(self.units(24), self.red)
            for p in range(3):
                for q in range(8):
                    rows = self.rows(p, q)
                    S[rows, :] += recv_d[p, self.at + q * self.blk:self.at + (q + 1) * self.blk, :]
            if self.t == 1:
                pl.semaphore_signal(ack.at[self.piece], inc=1, device_id=(partner,), device_id_type=MESH)
            for s in range(4):
                for p, (a, b, c) in self._orders():
                    self._pass(p, chips[a ^ (b + c, b, c, 0)[s]], 1 + s, a, rb1, p, s)

        def p2(self):
            for s in range(2):
                self._got(1 + s)
                for p, (a, b, c) in self._orders():
                    m = (b + c, b)[s]
                    self._add(p, chips[m], rb1, p, s)
                    self._pass(p, chips[m], 5 + s, b, rb2, p, s)

        def p2b(self):
            for s in (2, 3):
                self._got(1 + s)
                for p, (a, b, c) in self._orders():
                    self._add(p, chips[(c, 0)[s - 2]], rb1, p, s)

        def p3(self):
            self._got(5)
            for p, (a, b, c) in self._orders():
                self._add(p, chips[c], rb2, p, 0)
                self._pass(p, chips[c], 7, c, rb3, p)
            self._got(6)
            for p, (a, b, c) in self._orders():
                self._add(p, chips[0], rb2, p, 1)

        def p4(self):
            self._got(7)
            for p in range(3):
                rows = self.rows(p, chips[0])
                grads[rows, :] = S[rows, :] + self._buf(rb3, p)[...]
            self.start()

    class Push:
        def __init__(self, buf):
            self.buf, self.ssem, self.rsem = buf, new_sems(0, 1), new_sems(1, 1)

        def start(self):
            for i in range(1, NDEV):
                send(self.buf.at[me], self.buf.at[me], self.ssem, self.rsem, lax.rem(me + i, NDEV))

        def wait(self):
            arrived(self.buf.at[pl.ds(0, NDEV - 1)], self.rsem)

        def finish(self):
            sent(self.buf.at[pl.ds(0, NDEV - 1)], self.ssem)

    def order(i):
        return 4 - 2 * i + lax.div(i * (i - 1), 2)

    def device_of(slot):
        g = lax.div(slot + 1, 3)
        i = lax.rem(slot + 1, 3)
        near = order(i)
        m = jnp.where(slot < 2, 0, jnp.where(g < 3, near, jnp.where(g < 5, 7 - near, 7)))
        oth = jnp.where(slot < 2, slot, jnp.where(slot < 14, lax.rem(g - 1, 2), slot - 14))
        k = core + oth - 2 * core * oth
        return flip(m) * 2 + k

    def rowsl(q):
        return pl.ds(pl.multiple_of(q * R, R), R)

    def diag(r0, t):
        return (lax.broadcasted_iota(jnp.int32, (CH, L), 0) + r0
                == lax.broadcasted_iota(jnp.int32, (CH, L), 1) + L * t)

    def row_dot(slot):
        s512 = dot(u_all[rowsl(me), :], v_all[rowsl(device_of(slot)), :], NT)
        for t in range(4):
            S[(slot * 4 + t) * R:(slot * 4 + t + 1) * R, :] = s512[:, L * t:L * t + L]

    def row_rest(slot):
        q = device_of(slot)
        own = slot == 0
        for r0 in range(0, R, CH):
            rs = slice(r0, r0 + CH)
            idc = idcol[rs, :]
            vals = []
            pos = jnp.zeros((CH, L), F32)
            for t in range(4):
                off = slice((slot * 4 + t) * R + r0, (slot * 4 + t) * R + r0 + CH)
                s = S[off, :] * SCALE - lq_all[q, t:t + 1, :]
                hit = idc == ids_all[q, t:t + 1, :]
                if own:
                    dg = diag(r0, t)
                    pos = pos + jnp.where(dg, s, 0.0)
                    hit = jnp.logical_and(hit, jnp.logical_not(dg))
                s = jnp.where(hit, -jnp.inf, s)
                S[off, :] = s
                vals.append(s)
            mn = jnp.maximum(jnp.maximum(vals[0], vals[1]), jnp.maximum(vals[2], vals[3]))
            if own:
                pos_ref[rs, :] = pos
                mn = jnp.maximum(mn, LOWEST)
                tot = jnp.zeros((CH, L), F32)
            else:
                mo = m_ref[rs, :]
                mn = jnp.maximum(mn, mo)
                tot = l_ref[rs, :] * jnp.exp(mo - mn)
            for s in vals:
                tot = tot + jnp.exp(s - mn)
            l_ref[rs, :] = tot
            m_ref[rs, :] = mn

    def row_slots(a, b):
        row_dot(a)
        for slot in range(a, b):
            if slot + 1 < b:
                row_dot(slot + 1)
            row_rest(slot)

    def row_finish():
        m = m_ref[...]
        top = jnp.max(m, axis=1, keepdims=True)
        tot = jnp.sum(l_ref[...] * jnp.exp(m - top), axis=1, keepdims=True)
        inv = 1.0 / (tot * float(B))
        cost = top + jnp.log(tot) - jnp.sum(pos_ref[...], axis=1, keepdims=True)
        m_ref[...] = jnp.broadcast_to(top, (R, L))
        l_ref[...] = jnp.broadcast_to(inv, (R, L))
        lane = lax.broadcasted_iota(jnp.int32, (R, L), 1)
        pack = jnp.where(lane == 0, top, jnp.where(lane == 1, inv, jnp.where(lane == 2, cost, 0.0)))
        st_all[me] = pack.T[0:8, :]

    def du_fill(slot, k, own=False):
        for r0 in range(0, R, CH):
            rs = slice(r0, r0 + CH)
            mc = m_ref[rs, :]
            ic = l_ref[rs, :]
            for t in range(4):
                off = pl.ds(pl.multiple_of((slot * 4 + t) * R + r0, CH), CH)
                g = jnp.exp(S[off, :] - mc) * ic
                if own:
                    g = g - jnp.where(diag(r0, t), 1.0 / B, 0.0)
                G[k, rs, L * t:L * t + L] = g.astype(BF16)

    def du_dot(slot, k):
        acc[...] += dot(G[k], v_all[rowsl(device_of(slot)), :])

    def du_pairs(a, b):
        def pair(i, x):
            du_dot(2 * i, 0)
            du_fill(2 * i + 1, 1)
            du_dot(2 * i + 1, 1)
            du_fill(2 * i + 2, 0)
            return x
        lax.fori_loop(a, b, pair, 0)

    def dv_slot(slot, own):
        q = me if own else device_of(slot)
        big[...] = dot(v_all[rowsl(me), :], u_all[rowsl(q), :], NT)

        def chunk(r, _):
            r0 = pl.multiple_of(r * CH, CH)
            rs = pl.ds(r0, CH)
            idc = idcol[rs, :]
            lqc = lqcol[rs, :]
            for t in range(4):
                cs = slice(L * t, L * t + L)
                s = big[rs, cs] * SCALE - lqc
                hit = idc == ids_all[q, t:t + 1, :]
                if own:
                    dg = diag(r0, t)
                    hit = jnp.logical_and(hit, jnp.logical_not(dg))
                g = jnp.exp(jnp.where(hit, -jnp.inf, s) - st_all[q, 0:1, cs]) * st_all[q, 1:2, cs]
                if own:
                    g = g - jnp.where(dg, 1.0 / B, 0.0)
                G[0, rs, cs] = g.astype(BF16)
            return 0
        lax.fori_loop(0, R // CH, chunk, 0)
        part = dot(G[0], u_all[rowsl(q), :])
        acc[...] = part if own else acc[...] + part

    def dv_slots(a, b):
        lax.fori_loop(a, b, lambda s, c: (dv_slot(s, False), c)[1], 0)

    def put(t, r0, val):
        n = val.shape[0]
        for p in range(3):
            S[pl.ds(pl.multiple_of(wrow(t, p, 0) + r0, 8), n), :] = val[:, L * p:L * p + L]

    def backward(t, reds, hooks):
        d = acc[...] * SCALE
        e = e_ref[t]
        inv = inv_ref[t]
        s = jnp.sum(e * d, axis=1, keepdims=True)
        dzb = ((d - e * s) * jnp.concatenate([inv, inv, inv], axis=1)).astype(BF16)
        g3 = dot(h2[t], dzb, TN)
        put(t, 2 * D, g3[:D // 2])
        put(t, HALF + 2 * D, g3[D // 2:])
        da2 = jnp.where(h2[t] > 0, dot(dzb, w3b[t], NT), 0.0).astype(BF16)
        G[0, :, 0:D] = da2

        def mid(i):
            c = lax.rem(i + 2 * (1 - core), 4)
            base = lax.div(c, 2) * HALF + lax.rem(c, 2) * SEG
            cols = pl.ds(pl.multiple_of(c * D, L), D)
            g2 = G[0, :, 0:D]
            put(t, base, dot(h1[t, :, cols], g2, TN))
            g1 = dot(g2, w2b[t, cols, :], NT)
            da1[...] = jnp.where(h1[t, :, cols] > 0, g1, 0.0).astype(BF16)
            put(t, base + D, dot(xb[t], da1[...], TN))

        hooks[0]()
        mid(0)
        hooks[1]()
        reds[0].cross()
        mid(1)
        hooks[2]()
        reds[1].cross()
        lax.fori_loop(2, 4, lambda i, x: (mid(i), x)[1], 0)

    pi, pq, ps = Push(ids_all), Push(lq_all), Push(st_all)
    ua, ub, ia, ib = Reduce(1, 0), Reduce(1, 1), Reduce(0, 0), Reduce(0, 1)

    def nothing():
        pass

    forward(0, v_all)
    pl.semaphore_wait(barrier, NDEV - 1)
    gv.start()
    pi.start()
    pq.start()
    forward(1, u_all)
    gv.f1()
    pi.wait()
    pq.wait()
    gv.other(0)
    row_slots(0, 2)
    gv.f2()
    gv.f2b()
    row_slots(2, 5)
    gv.f3()
    gu.start()
    gv.other(1)
    row_slots(5, 8)
    gv.f4()
    row_slots(8, 11)
    gv.f5()
    gv.other(2)
    row_slots(11, 15)
    gv.other(3)
    row_slots(15, 16)
    row_finish()
    ps.start()
    gu.f1()
    gu.f2()
    acc[...] = jnp.zeros((R, D), F32)
    du_fill(0, 0, True)
    du_pairs(0, 3)
    gu.f2b()
    du_pairs(3, 7)
    du_dot(14, 0)
    du_fill(15, 1)
    du_dot(15, 1)
    backward(1, (ua, ub), (nothing, gu.f3, nothing))
    ua.p1()
    gu.f4()
    ub.p1()
    ps.wait()
    gu.other(0)
    gu.other(1)
    dv_slot(0, True)
    gu.f5()
    dv_slots(1, 4)
    ua.p2()
    dv_slots(4, 6)
    ua.p2b()
    gu.other(2)
    gu.other(3)
    dv_slots(6, 8)
    ub.p2()
    dv_slots(8, 9)
    ub.p2b()
    dv_slots(9, 10)
    ua.p3()
    dv_slots(10, 12)
    ub.p3()
    dv_slots(12, 13)
    ua.p4()
    dv_slots(13, 15)
    ub.p4()
    dv_slots(15, 16)

    def turn(i):
        def go():
            (ua, ub)[i].f1()
            pl.semaphore_wait(ack.at[i], 1)
        return go

    backward(0, (ia, ib), (nothing, turn(0), turn(1)))
    ua.f2()
    ia.p1()
    ub.f2()
    ib.p1()
    ua.f2b()
    ua.f3()
    ia.p2()
    ub.f2b()
    ub.f3()
    ia.p2b()
    ib.p2()
    ib.p2b()
    ua.f4()
    ia.p3()
    ub.f4()
    ib.p3()
    ia.p4()
    ua.f5()
    ib.p4()
    ub.f5()
    total = jnp.sum(jnp.sum(st_all[...], axis=0)[2:3, :]) * (1.0 / B)
    loss[0, 0] = total
    ia.f1()
    ia.f2()
    ib.f1()
    ib.f2()
    ua.other()
    ub.other()
    ia.f2b()
    ia.f3()
    ib.f2b()
    ib.f3()
    ia.f4()
    ib.f4()
    ia.f5()
    ib.f5()
    ia.other()
    ib.other()
    for x in (gv, gu, pi, pq, ps, ua, ub, ia, ib):
        x.finish()


def write_kernel(loss_in, grads, loss, gu1, gu2, gu3, gi1, gi2, gi3, sem):
    loss[0, 0] = loss_in[0, 0]
    for t, (g1, g2, g3) in enumerate(((gi1, gi2, gi3), (gu1, gu2, gu3))):
        for p in range(3):
            pc = pl.ds(L * p, L)
            for h in range(2):
                o = t * WROWS + p * PACK + h * HALF
                jobs = [(o + 2 * D, g3.at[pl.ds(h * (D // 2), D // 2), pc])]
                for i in range(2):
                    c = 2 * h + i
                    jobs.append((o + i * SEG, g2.at[pl.ds(D * c, D), pc]))
                    jobs.append((o + i * SEG + D, g1.at[:, pl.ds(D * c + L * p, L)]))
                for r0, dst in jobs:
                    src = grads.at[pl.ds(r0, dst.shape[0]), :]
                    pltpu.make_async_copy(src, dst, sem).start()
    pltpu.make_async_copy(grads, grads, sem).wait()


def solution(mesh):
    vm = pl.BlockSpec(memory_space=pltpu.VMEM)
    sm = pl.BlockSpec(memory_space=pltpu.SMEM)
    hbm = pl.BlockSpec(memory_space=pl.ANY)
    shp = jax.ShapeDtypeStruct

    def device_step(user_x, item_x, item_id, log_q, user_w1, user_w2, user_w3, item_w1, item_w2, item_w3):
        V = pltpu.VMEM
        loss, grads = pl.pallas_call(
            kernel,
            out_shape=(shp((1, 1), F32), V((2 * WROWS, L), F32)),
            in_specs=[hbm, hbm, vm, vm] + [hbm] * 6,
            out_specs=(sm, vm),
            scratch_shapes=[
                V((64 * R, L), F32), V((B, D), BF16), V((B, D), BF16),
                V((2, R, D), BF16), V((2, R, H), BF16), V((2, R, D), BF16),
                V((2, R, D), F32), V((2, R, L), F32),
                V((2, D, H), BF16), V((2, H, D), BF16), V((2, D, D), BF16), V((R, D), BF16),
                V((NDEV, 4, L), jnp.int32), V((NDEV, 4, L), F32), V((NDEV, 8, R), F32),
                V((R, L), jnp.int32), V((R, L), F32), V((R, L), F32), V((R, L), F32), V((R, L), F32),
                V((2, R, R), BF16), V((R, D), F32), V((R, R), F32),
                V((3, HALF, L), F32), V((3, 4, BLK, L), F32), V((3, 2, BLK, L), F32),
                V((3, BLK, L), F32),
                pltpu.SemaphoreType.DMA((N_SEND,)), pltpu.SemaphoreType.DMA((N_RECV,)),
                pltpu.SemaphoreType.DMA((2, 6)), pltpu.SemaphoreType.REGULAR((2,)),
            ],
            compiler_params=pltpu.CompilerParams(collective_id=0, has_side_effects=True,
                                                 vmem_limit_bytes=VMEM_LIMIT),
            name='step',
        )(user_x, item_x, item_id.reshape(4, L), log_q.reshape(4, L),
          user_w1, user_w2, user_w3, item_w1, item_w2, item_w3)
        out = pl.pallas_call(
            write_kernel,
            out_shape=(shp((1, 1), F32), shp((D, H), F32), shp((H, D), F32), shp((D, D), F32),
                       shp((D, H), F32), shp((H, D), F32), shp((D, D), F32)),
            in_specs=[sm, vm],
            out_specs=(sm,) + (hbm,) * 6,
            scratch_shapes=[pltpu.SemaphoreType.DMA],
            compiler_params=pltpu.CompilerParams(vmem_limit_bytes=1 << 20),
            name='write',
        )(loss, grads)
        return (out[0].reshape(()),) + tuple(out[1:])

    batch_spec = P('dp', None)
    vec_spec = P('dp')
    whole = P()
    return jax.shard_map(device_step, mesh=mesh,
                         in_specs=(batch_spec, batch_spec, vec_spec, vec_spec, whole, whole, whole, whole, whole, whole),
                         out_specs=(whole,) * 7, check_vma=False)
```

```python
import jax
import jax.numpy as jnp
from jax import lax
from jax.experimental import pallas as pl
from jax.experimental.pallas import tpu as pltpu
from jax.sharding import PartitionSpec as P

SCALE = 20.0
EPS = 1e-6
NDEV = 16
R = 512
D = 384
H = 1536
B = R * NDEV
BLK = 216
HALF = 8 * BLK
N_SEND, N_RECV = 9, 89
PACK = 2 * HALF
SEG = 960
WROWS = 3 * PACK
L = 128
CH = 64
VMEM_LIMIT = 56000000
F32, BF16 = jnp.float32, jnp.bfloat16
MESH = pl.DeviceIdType.MESH
NT = (((1,), (1,)), ((), ()))
TN = (((0,), (0,)), ((), ()))
LOWEST = float(jnp.finfo(jnp.float32).min)
DIMS = (4, 2, 1)
CROSS = ((0,), (4, 2, 1), (6, 5, 3), (7,))


def dot(a, b, dims=(((1,), (0,)), ((), ()))):
    return lax.dot_general(a, b, dims, preferred_element_type=F32)


def kernel(ux, ix, ids_in, lq_in, uw1, uw2, uw3, iw1, iw2, iw3,
           loss, grads,
           S, v_all, u_all, xb, h1, h2, e_ref, inv_ref, w1b, w2b, w3b, da1,
           ids_all, lq_all, st_all, idcol, lqcol, m_ref, l_ref, pos_ref, G, acc, big,
           recv_d, rb1, rb2, rb3, send_sem, recv_sem, loc_sem, ack, hello):
    made = [0, 0]

    def new_sems(kind, n):
        made[kind] += n
        return made[kind] - n

    me = lax.axis_index('dp')
    core = lax.rem(me, 2)
    chip = lax.div(me, 2)
    partner = me + 1 - 2 * core

    def flip(m):
        out = 0
        for d in DIMS:
            bit = lax.rem(lax.div(chip, d), 2)
            if isinstance(m, int):
                f = (m // d) % 2
            else:
                f = lax.rem(lax.div(m, d), 2)
            out = out + d * (bit + f - 2 * bit * f)
        return out

    chips = [flip(m) for m in range(8)]

    def nbr(d):
        return chips[d] * 2 + core

    def rc(src, dst, ssem, rsem, dev):
        return pltpu.make_async_remote_copy(src, dst, send_sem.at[ssem], recv_sem.at[rsem],
                                            device_id=(dev,), device_id_type=MESH)

    def send(src, dst, ssem, rsem, dev):
        rc(src, dst, ssem, rsem, dev).start()

    def arrived(ref, rsem):
        rc(ref, ref, 0, rsem, partner).wait_recv()

    def sent(ref, ssem):
        rc(ref, ref, ssem, 0, partner).wait_send()

    near = [partner] + [nbr(d) for d in DIMS]

    def greet(sem):
        for n in near:
            pl.semaphore_signal(sem, inc=1, device_id=(n,), device_id_type=MESH)

    def greeted(i):
        pl.semaphore_wait(hello.at[i], len(near))
        if i < 2:
            greet(hello.at[i + 1])

    barrier = pltpu.get_barrier_semaphore()
    greet(barrier)

    def load(src, dst, t, k):
        pltpu.make_async_copy(src, dst, loc_sem.at[t, k]).start()

    def loaded(t, k, o, n):
        ref = S.at[pl.ds(o, n), :]
        pltpu.make_async_copy(ref, ref, loc_sem.at[t, k]).wait()

    W2_AT, W3_AT, STAGE = 12 * D, 12 * D + 3 * H, WROWS + 3 * R

    def start_loads(t, xr, w1, w2, w3):
        o = t * STAGE

        def columns(src, at, rows, c, k):
            load(src.at[:, pl.ds(L * c, L)], S.at[pl.ds(o + at + rows * c, rows), :], t, k)
        for c in range(3):
            columns(xr, WROWS, R, c, 0)
        for c in range(12):
            columns(w1, 0, D, c, 1 + c // 4)
        for c in range(3):
            columns(w2, W2_AT, H, c, 4)
        for c in range(3):
            columns(w3, W3_AT, D, c, 5)

    start_loads(0, ix, iw1, iw2, iw3)
    load(ids_in, ids_all.at[me], 0, 6)
    load(lq_in, lq_all.at[me], 1, 6)

    def columns_of_ids():
        pltpu.make_async_copy(ids_in, ids_all.at[me], loc_sem.at[0, 6]).wait()
        pltpu.make_async_copy(lq_in, lq_all.at[me], loc_sem.at[1, 6]).wait()
        for t in range(4):
            idcol[L * t:L * t + L, :] = jnp.broadcast_to(ids_all[me, t:t + 1, :], (L, L)).T
            lqcol[L * t:L * t + L, :] = jnp.broadcast_to(lq_all[me, t:t + 1, :], (L, L)).T

    def forward(t, dest, greeting):
        o = t * STAGE

        def take(dst, at, rows, c):
            dst[t, :, L * c:L * c + L] = S[o + at + rows * c:o + at + rows * (c + 1), :].astype(BF16)

        loaded(t, 0, o + WROWS, 3 * R)
        for c in range(3):
            take(xb, WROWS, R, c)
        for n in range(3):
            loaded(t, 1 + n, o + 4 * n * D, 4 * D)
            for c in range(4):
                take(w1b, 0, D, 4 * n + c)
            cols = slice(4 * n * L, 4 * (n + 1) * L)
            h1[t, :, cols] = jnp.maximum(dot(xb[t], w1b[t, :, cols]), 0.0).astype(BF16)
        if greeting:
            greeted(0)
        loaded(t, 4, o + W2_AT, 3 * H)
        if t == 0:
            start_loads(1, ux, uw1, uw2, uw3)
        for c in range(3):
            take(w2b, W2_AT, H, c)
        h2[t] = jnp.maximum(dot(h1[t], w2b[t]), 0.0).astype(BF16)
        if greeting:
            greeted(1)
        loaded(t, 5, o + W3_AT, 3 * D)
        for c in range(3):
            take(w3b, W3_AT, D, c)
        z = dot(h2[t], w3b[t])
        inv = lax.rsqrt(jnp.sum(z * z, axis=1, keepdims=True) + EPS)
        inv_ref[t] = jnp.broadcast_to(inv, (R, L))
        e = z * inv
        e_ref[t] = e
        dest[pl.ds(pl.multiple_of(me * R, R), R), :] = e.astype(BF16)

    class Gather:
        def __init__(self, part, full, units, ssem):
            self.part, self.full, self.units, self.ssem = part, full, units, ssem
            self.rsem = new_sems(1, 7)
            self.other_sem = None

        def _each(self, rel):
            for p in range(3):
                o = [DIMS[(p + i) % 3] for i in range(3)]
                yield p, o, self.part(p, chips[sum(o[i] for i in rel)])

        def _send(self, j, pos, rel):
            for p, o, r in self._each(rel):
                send(r, r, self.ssem, self.rsem + j, nbr(o[pos]))

        def _wait(self, j):
            arrived(self.units(3), self.rsem + j)

        def _cross(self, g):
            if self.other_sem is None:
                self.other_sem = self.cross_sems()
            for m in CROSS[g]:
                for r in self.full(chips[m]):
                    send(r, r, self.ssem, self.other_sem[g], partner)

        def start(self):
            self._send(0, 0, ())
            self._send(1, 1, ())
            self._send(3, 2, ())
            self._cross(0)

        def f1(self):
            self._wait(0)
            self._send(2, 1, (0,))
            self._send(4, 2, (0,))

        def f2(self):
            self._wait(1)
            self._send(5, 2, (1,))

        def f2b(self):
            self._wait(3)
            self._cross(1)

        def f3(self):
            self._wait(2)
            self._send(6, 2, (0, 1))

        def f4(self):
            self._wait(4)
            self._wait(5)
            self._cross(2)

        def f5(self):
            self._wait(6)
            self._cross(3)

    class Embeddings(Gather):
        def __init__(self, buf):
            def rows(c):
                return pl.ds(pl.multiple_of((c * 2 + core) * R, R), R)
            self.buf = buf
            super().__init__(lambda p, c: buf.at[rows(c), pl.ds(L * p, L)], lambda c: (buf.at[rows(c), :],),
                             lambda n: buf.at[pl.ds(0, n // 3 * R), :], new_sems(0, 1))

        def cross_sems(self):
            k = new_sems(1, 4)
            return range(k, k + 4)

        def other(self, g):
            arrived(self.units(3 * len(CROSS[g])), self.other_sem[g])

        def finish(self):
            sent(self.units(3 * (NDEV - 1)), self.ssem)

    gv = Embeddings(v_all)
    gu = Embeddings(u_all)

    def wrow(t, p, r):
        return t * WROWS + p * PACK + r

    class Reduce(Gather):
        def __init__(self, t, piece):
            self.t, self.piece = t, piece
            self.at, self.blk = ((0, SEG // 8), (SEG, (HALF - SEG) // 8))[piece]
            self.sub = (0, SEG // 8)[piece]
            super().__init__(lambda p, c: grads.at[self.rows(p, c), :], self._all_parts,
                             lambda n: grads.at[pl.ds(0, n * self.blk), :], new_sems(0, 1))
            self.red = new_sems(1, 8)

        def rows(self, p, c):
            return pl.ds(pl.multiple_of(wrow(self.t, p, 0) + core * HALF + self.at + c * self.blk, 8), self.blk)

        def _all_parts(self, c):
            return [grads.at[self.rows(p, c), :] for p in range(3)]

        def cross_sems(self):
            return (new_sems(1, 1),) * 4

        def other(self):
            arrived(self.units(24), self.other_sem[0])

        def finish(self):
            sent(self.units(90), self.ssem)

        def cross(self):
            n = 8 * self.blk
            for p in range(3):
                rows = pl.ds(pl.multiple_of(wrow(self.t, p, 0) + (1 - core) * HALF + self.at, 8), n)
                send(S.at[rows, :], recv_d.at[p, pl.ds(self.at, n), :], self.ssem, self.red, partner)

        def _orders(self):
            for p in range(3):
                yield p, [DIMS[(p + i) % 3] for i in range(3)]

        def _got(self, k):
            arrived(self.units(3), self.red + k)

        def _buf(self, ref, *i):
            return ref.at[(*i, pl.ds(self.sub, self.blk), slice(None))]

        def _add(self, p, c, ref, *i):
            rows = self.rows(p, c)
            S[rows, :] += self._buf(ref, *i)[...]

        def _pass(self, p, c, k, dev, ref, *i):
            send(S.at[self.rows(p, c), :], self._buf(ref, *i), self.ssem, self.red + k, nbr(dev))

        def p1(self):
            arrived(self.units(24), self.red)
            for p in range(3):
                for q in range(8):
                    rows = self.rows(p, q)
                    S[rows, :] += recv_d[p, self.at + q * self.blk:self.at + (q + 1) * self.blk, :]
            if self.t == 1:
                pl.semaphore_signal(ack.at[self.piece], inc=1, device_id=(partner,), device_id_type=MESH)
            self._first(0)

        def _first(self, h):
            for s in (2 * h, 2 * h + 1):
                for p, (a, b, c) in self._orders():
                    self._pass(p, chips[a ^ (b + c, b, c, 0)[s]], 1 + s, a, rb1, p, s)

        def p1b(self):
            self._first(1)

        def p2(self):
            for s in range(2):
                self._got(1 + s)
                for p, (a, b, c) in self._orders():
                    m = (b + c, b)[s]
                    self._add(p, chips[m], rb1, p, s)
                    self._pass(p, chips[m], 5 + s, b, rb2, p, s)

        def p2b(self):
            for s in (2, 3):
                self._got(1 + s)
                for p, (a, b, c) in self._orders():
                    self._add(p, chips[(c, 0)[s - 2]], rb1, p, s)

        def p3(self):
            self._got(5)
            for p, (a, b, c) in self._orders():
                self._add(p, chips[c], rb2, p, 0)
                self._pass(p, chips[c], 7, c, rb3, p)

        def p3b(self):
            self._got(6)
            for p, (a, b, c) in self._orders():
                self._add(p, chips[0], rb2, p, 1)

        def p4(self):
            self._got(7)
            for p in range(3):
                rows = self.rows(p, chips[0])
                grads[rows, :] = S[rows, :] + self._buf(rb3, p)[...]
            self.start()

    class Push:
        def __init__(self, buf):
            self.buf, self.ssem, self.rsem = buf, new_sems(0, 1), new_sems(1, 1)

        def start(self):
            for i in range(1, NDEV):
                send(self.buf.at[me], self.buf.at[me], self.ssem, self.rsem, lax.rem(me + i, NDEV))

        def wait(self):
            arrived(self.buf.at[pl.ds(0, NDEV - 1)], self.rsem)

        def finish(self):
            sent(self.buf.at[pl.ds(0, NDEV - 1)], self.ssem)

    def order(i):
        return 4 - 2 * i + lax.div(i * (i - 1), 2)

    def device_of(slot):
        g = lax.div(slot + 1, 3)
        i = lax.rem(slot + 1, 3)
        near = order(i)
        m = jnp.where(slot < 2, 0, jnp.where(g < 3, near, jnp.where(g < 5, 7 - near, 7)))
        oth = jnp.where(slot < 2, slot, jnp.where(slot < 14, lax.rem(g - 1, 2), slot - 14))
        k = core + oth - 2 * core * oth
        return flip(m) * 2 + k

    def rowsl(q):
        return pl.ds(pl.multiple_of(q * R, R), R)

    def diag(r0, t):
        return (lax.broadcasted_iota(jnp.int32, (CH, L), 0) + r0
                == lax.broadcasted_iota(jnp.int32, (CH, L), 1) + L * t)

    def row_dot(slot):
        s512 = dot(u_all[rowsl(me), :], v_all[rowsl(device_of(slot)), :], NT)
        for t in range(4):
            S[(slot * 4 + t) * R:(slot * 4 + t + 1) * R, :] = s512[:, L * t:L * t + L]

    def row_rest(slot):
        q = device_of(slot)
        own = slot == 0
        for r0 in range(0, R, CH):
            rs = slice(r0, r0 + CH)
            idc = idcol[rs, :]
            vals = []
            pos = jnp.zeros((CH, L), F32)
            for t in range(4):
                off = slice((slot * 4 + t) * R + r0, (slot * 4 + t) * R + r0 + CH)
                s = S[off, :] * SCALE - lq_all[q, t:t + 1, :]
                hit = idc == ids_all[q, t:t + 1, :]
                if own:
                    dg = diag(r0, t)
                    pos = pos + jnp.where(dg, s, 0.0)
                    hit = jnp.logical_and(hit, jnp.logical_not(dg))
                s = jnp.where(hit, -jnp.inf, s)
                S[off, :] = s
                vals.append(s)
            mn = jnp.maximum(jnp.maximum(vals[0], vals[1]), jnp.maximum(vals[2], vals[3]))
            if own:
                pos_ref[rs, :] = pos
                mn = jnp.maximum(mn, LOWEST)
                tot = jnp.zeros((CH, L), F32)
            else:
                mo = m_ref[rs, :]
                mn = jnp.maximum(mn, mo)
                tot = l_ref[rs, :] * jnp.exp(mo - mn)
            for s in vals:
                tot = tot + jnp.exp(s - mn)
            l_ref[rs, :] = tot
            m_ref[rs, :] = mn

    def row_slots(a, b):
        row_dot(a)
        for slot in range(a, b):
            if slot + 1 < b:
                row_dot(slot + 1)
            row_rest(slot)

    def row_finish():
        m = m_ref[...]
        top = jnp.max(m, axis=1, keepdims=True)
        tot = jnp.sum(l_ref[...] * jnp.exp(m - top), axis=1, keepdims=True)
        inv = 1.0 / (tot * float(B))
        cost = top + jnp.log(tot) - jnp.sum(pos_ref[...], axis=1, keepdims=True)
        m_ref[...] = jnp.broadcast_to(top, (R, L))
        l_ref[...] = jnp.broadcast_to(inv, (R, L))
        lane = lax.broadcasted_iota(jnp.int32, (R, L), 1)
        pack = jnp.where(lane == 0, top, jnp.where(lane == 1, inv, jnp.where(lane == 2, cost, 0.0)))
        st_all[me] = pack.T[0:8, :]

    def du_fill(slot, k, own=False):
        for r0 in range(0, R, CH):
            rs = slice(r0, r0 + CH)
            mc = m_ref[rs, :]
            ic = l_ref[rs, :]
            for t in range(4):
                off = pl.ds(pl.multiple_of((slot * 4 + t) * R + r0, CH), CH)
                g = jnp.exp(S[off, :] - mc) * ic
                if own:
                    g = g - jnp.where(diag(r0, t), 1.0 / B, 0.0)
                G[k, rs, L * t:L * t + L] = g.astype(BF16)

    def du_dot(slot, k):
        acc[...] += dot(G[k], v_all[rowsl(device_of(slot)), :])

    def du_pairs(a, b):
        def pair(i, x):
            du_dot(2 * i, 0)
            du_fill(2 * i + 1, 1)
            du_dot(2 * i + 1, 1)
            du_fill(2 * i + 2, 0)
            return x
        lax.fori_loop(a, b, pair, 0)

    def dv_slot(slot, own):
        q = me if own else device_of(slot)
        big[...] = dot(v_all[rowsl(me), :], u_all[rowsl(q), :], NT)

        def chunk(r, _):
            r0 = pl.multiple_of(r * CH, CH)
            rs = pl.ds(r0, CH)
            idc = idcol[rs, :]
            lqc = lqcol[rs, :]
            for t in range(4):
                cs = slice(L * t, L * t + L)
                s = big[rs, cs] * SCALE - lqc
                hit = idc == ids_all[q, t:t + 1, :]
                if own:
                    dg = diag(r0, t)
                    hit = jnp.logical_and(hit, jnp.logical_not(dg))
                g = jnp.exp(jnp.where(hit, -jnp.inf, s) - st_all[q, 0:1, cs]) * st_all[q, 1:2, cs]
                if own:
                    g = g - jnp.where(dg, 1.0 / B, 0.0)
                G[0, rs, cs] = g.astype(BF16)
            return 0
        lax.fori_loop(0, R // CH, chunk, 0)
        part = dot(G[0], u_all[rowsl(q), :])
        acc[...] = part if own else acc[...] + part

    def dv_slots(a, b):
        lax.fori_loop(a, b, lambda s, c: (dv_slot(s, False), c)[1], 0)

    def put(t, r0, val):
        n = val.shape[0]
        for p in range(3):
            S[pl.ds(pl.multiple_of(wrow(t, p, 0) + r0, 8), n), :] = val[:, L * p:L * p + L]

    def backward(t, reds, hooks):
        d = acc[...] * SCALE
        e = e_ref[t]
        inv = inv_ref[t]
        s = jnp.sum(e * d, axis=1, keepdims=True)
        dzb = ((d - e * s) * jnp.concatenate([inv, inv, inv], axis=1)).astype(BF16)
        g3 = dot(h2[t], dzb, TN)
        put(t, 2 * D, g3[:D // 2])
        put(t, HALF + 2 * D, g3[D // 2:])
        da2 = jnp.where(h2[t] > 0, dot(dzb, w3b[t], NT), 0.0).astype(BF16)
        G[0, :, 0:D] = da2

        def mid(i):
            c = lax.rem(i + 2 * (1 - core), 4)
            base = lax.div(c, 2) * HALF + lax.rem(c, 2) * SEG
            cols = pl.ds(pl.multiple_of(c * D, L), D)
            g2 = G[0, :, 0:D]
            put(t, base, dot(h1[t, :, cols], g2, TN))
            g1 = dot(g2, w2b[t, cols, :], NT)
            da1[...] = jnp.where(h1[t, :, cols] > 0, g1, 0.0).astype(BF16)
            put(t, base + D, dot(xb[t], da1[...], TN))

        hooks[0]()
        mid(0)
        hooks[1]()
        reds[0].cross()
        mid(1)
        hooks[2]()
        reds[1].cross()
        lax.fori_loop(2, 4, lambda i, x: (mid(i), x)[1], 0)

    pi, pq, ps = Push(ids_all), Push(lq_all), Push(st_all)
    ua, ub, ia, ib = Reduce(1, 0), Reduce(1, 1), Reduce(0, 0), Reduce(0, 1)

    def nothing():
        pass

    forward(0, v_all, False)
    pl.semaphore_wait(barrier, len(near))
    gv.start()
    greet(hello.at[0])
    columns_of_ids()
    forward(1, u_all, True)
    greeted(2)
    pi.start()
    pq.start()
    gv.f1()
    pi.wait()
    pq.wait()
    gv.other(0)
    row_slots(0, 2)
    gv.f2()
    gv.f2b()
    row_slots(2, 5)
    gv.f3()
    gu.start()
    gv.other(1)
    row_slots(5, 8)
    gv.f4()
    row_slots(8, 11)
    gv.f5()
    gv.other(2)
    row_slots(11, 15)
    gv.other(3)
    row_slots(15, 16)
    row_finish()
    ps.start()
    gu.f1()
    gu.f2()
    acc[...] = jnp.zeros((R, D), F32)
    du_fill(0, 0, True)
    du_pairs(0, 3)
    gu.f2b()
    du_pairs(3, 7)
    du_dot(14, 0)
    du_fill(15, 1)
    du_dot(15, 1)
    backward(1, (ua, ub), (nothing, gu.f3, nothing))
    ua.p1()
    ua.p1b()
    ub.p1()
    gu.f4()
    ps.wait()
    gu.other(0)
    gu.other(1)
    dv_slot(0, True)
    dv_slots(1, 4)
    ua.p2()
    ub.p1b()
    gu.f5()
    dv_slots(4, 6)
    ua.p2b()
    gu.other(2)
    dv_slots(6, 9)
    ua.p3()
    ub.p2()
    dv_slots(9, 10)
    ua.p3b()
    gu.other(3)
    dv_slots(10, 11)
    ub.p2b()
    dv_slots(11, 12)
    ua.p4()
    dv_slots(12, 13)
    ub.p3()
    dv_slots(13, 15)
    ub.p3b()
    dv_slots(15, 16)
    ub.p4()

    def turn(i):
        def go():
            if i == 0:
                ua.f1()
            pl.semaphore_wait(ack.at[i], 1)
        return go

    backward(0, (ia, ib), (nothing, turn(0), turn(1)))
    ua.f2()
    ia.p1()
    ia.p1b()
    ub.f1()
    ib.p1()
    ib.p1b()
    ua.f2b()
    ia.p2()
    ua.f3()
    ub.f2()
    ia.p2b()
    ib.p2()
    ub.f2b()
    ub.f3()
    ib.p2b()
    ia.p3()
    ua.f4()
    ia.p3b()
    ib.p3()
    ub.f4()
    ib.p3b()
    ia.p4()
    ua.f5()
    ib.p4()
    ub.f5()
    total = jnp.sum(jnp.sum(st_all[...], axis=0)[2:3, :]) * (1.0 / B)
    loss[0, 0] = total
    ia.f1()
    ia.f2()
    ib.f1()
    ib.f2()
    ua.other()
    ub.other()
    ia.f2b()
    ia.f3()
    ib.f2b()
    ib.f3()
    ia.f4()
    ib.f4()
    ia.f5()
    ib.f5()
    ia.other()
    ib.other()
    for x in (gv, gu, pi, pq, ps, ua, ub, ia, ib):
        x.finish()


def write_kernel(loss_in, grads, loss, gu1, gu2, gu3, gi1, gi2, gi3, sem):
    loss[0, 0] = loss_in[0, 0]
    for t, (g1, g2, g3) in enumerate(((gi1, gi2, gi3), (gu1, gu2, gu3))):
        for p in range(3):
            pc = pl.ds(L * p, L)
            for h in range(2):
                o = t * WROWS + p * PACK + h * HALF
                jobs = [(o + 2 * D, g3.at[pl.ds(h * (D // 2), D // 2), pc])]
                for i in range(2):
                    c = 2 * h + i
                    jobs.append((o + i * SEG, g2.at[pl.ds(D * c, D), pc]))
                    jobs.append((o + i * SEG + D, g1.at[:, pl.ds(D * c + L * p, L)]))
                for r0, dst in jobs:
                    src = grads.at[pl.ds(r0, dst.shape[0]), :]
                    pltpu.make_async_copy(src, dst, sem).start()
    pltpu.make_async_copy(grads, grads, sem).wait()


def solution(mesh):
    vm = pl.BlockSpec(memory_space=pltpu.VMEM)
    sm = pl.BlockSpec(memory_space=pltpu.SMEM)
    hbm = pl.BlockSpec(memory_space=pl.ANY)
    shp = jax.ShapeDtypeStruct

    def device_step(user_x, item_x, item_id, log_q, user_w1, user_w2, user_w3, item_w1, item_w2, item_w3):
        V = pltpu.VMEM
        loss, grads = pl.pallas_call(
            kernel,
            out_shape=(shp((1, 1), F32), V((2 * WROWS, L), F32)),
            in_specs=[hbm] * 10,
            out_specs=(sm, vm),
            scratch_shapes=[
                V((64 * R, L), F32), V((B, D), BF16), V((B, D), BF16),
                V((2, R, D), BF16), V((2, R, H), BF16), V((2, R, D), BF16),
                V((2, R, D), F32), V((2, R, L), F32),
                V((2, D, H), BF16), V((2, H, D), BF16), V((2, D, D), BF16), V((R, D), BF16),
                V((NDEV, 4, L), jnp.int32), V((NDEV, 4, L), F32), V((NDEV, 8, R), F32),
                V((R, L), jnp.int32), V((R, L), F32), V((R, L), F32), V((R, L), F32), V((R, L), F32),
                V((2, R, R), BF16), V((R, D), F32), V((R, R), F32),
                V((3, HALF, L), F32), V((3, 4, BLK, L), F32), V((3, 2, BLK, L), F32),
                V((3, BLK, L), F32),
                pltpu.SemaphoreType.DMA((N_SEND,)), pltpu.SemaphoreType.DMA((N_RECV,)),
                pltpu.SemaphoreType.DMA((2, 7)), pltpu.SemaphoreType.REGULAR((2,)),
                pltpu.SemaphoreType.REGULAR((3,)),
            ],
            compiler_params=pltpu.CompilerParams(collective_id=0, has_side_effects=True,
                                                 vmem_limit_bytes=VMEM_LIMIT),
            name='step',
        )(user_x, item_x, item_id.reshape(4, L), log_q.reshape(4, L),
          user_w1, user_w2, user_w3, item_w1, item_w2, item_w3)
        out = pl.pallas_call(
            write_kernel,
            out_shape=(shp((1, 1), F32), shp((D, H), F32), shp((H, D), F32), shp((D, D), F32),
                       shp((D, H), F32), shp((H, D), F32), shp((D, D), F32)),
            in_specs=[sm, vm],
            out_specs=(sm,) + (hbm,) * 6,
            scratch_shapes=[pltpu.SemaphoreType.DMA],
            compiler_params=pltpu.CompilerParams(vmem_limit_bytes=1 << 20),
            name='write',
        )(loss, grads)
        return (out[0].reshape(()),) + tuple(out[1:])

    batch_spec = P('dp', None)
    vec_spec = P('dp')
    whole = P()
    return jax.shard_map(device_step, mesh=mesh,
                         in_specs=(batch_spec, batch_spec, vec_spec, vec_spec, whole, whole, whole, whole, whole, whole),
                         out_specs=(whole,) * 7, check_vma=False)
```

```python
import jax
import jax.numpy as jnp
from jax import lax
from jax.experimental import pallas as pl
from jax.experimental.pallas import tpu as pltpu
from jax.sharding import PartitionSpec as P

SCALE = 20.0
EPS = 1e-6
NDEV = 16
R = 512
D = 384
H = 1536
B = R * NDEV
BLK = 216
HALF = 8 * BLK
N_SEND, N_RECV = 9, 89
PACK = 2 * HALF
SEG = 960
WROWS = 3 * PACK
L = 128
CH = 64
VMEM_LIMIT = 56000000
F32, BF16 = jnp.float32, jnp.bfloat16
MESH = pl.DeviceIdType.MESH
NT = (((1,), (1,)), ((), ()))
TN = (((0,), (0,)), ((), ()))
LOWEST = float(jnp.finfo(jnp.float32).min)
DIMS = (4, 2, 1)
CROSS = ((0,), (4, 2, 1), (6, 5, 3), (7,))


def dot(a, b, dims=(((1,), (0,)), ((), ()))):
    return lax.dot_general(a, b, dims, preferred_element_type=F32)


def kernel(ux, ix, ids_in, lq_in, uw1, uw2, uw3, iw1, iw2, iw3,
           loss, grads,
           S, v_all, u_all, xb, h1, h2, e_ref, inv_ref, w1b, w2b, w3b, da1,
           ids_all, lq_all, st_all, idcol, lqcol, m_ref, l_ref, pos_ref, G, acc, big,
           recv_d, rb1, rb2, rb3, send_sem, recv_sem, loc_sem, ack, hello):
    made = [0, 0]

    def new_sems(kind, n):
        made[kind] += n
        return made[kind] - n

    me = lax.axis_index('dp')
    core = lax.rem(me, 2)
    chip = lax.div(me, 2)
    partner = me + 1 - 2 * core

    def flip(m):
        out = 0
        for d in DIMS:
            bit = lax.rem(lax.div(chip, d), 2)
            if isinstance(m, int):
                f = (m // d) % 2
            else:
                f = lax.rem(lax.div(m, d), 2)
            out = out + d * (bit + f - 2 * bit * f)
        return out

    chips = [flip(m) for m in range(8)]

    def nbr(d):
        return chips[d] * 2 + core

    def rc(src, dst, ssem, rsem, dev):
        return pltpu.make_async_remote_copy(src, dst, send_sem.at[ssem], recv_sem.at[rsem],
                                            device_id=(dev,), device_id_type=MESH)

    def send(src, dst, ssem, rsem, dev):
        rc(src, dst, ssem, rsem, dev).start()

    def arrived(ref, rsem):
        rc(ref, ref, 0, rsem, partner).wait_recv()

    def sent(ref, ssem):
        rc(ref, ref, ssem, 0, partner).wait_send()

    near = [partner] + [nbr(d) for d in DIMS]

    def greet(sem):
        for n in near:
            pl.semaphore_signal(sem, inc=1, device_id=(n,), device_id_type=MESH)

    def greeted(i):
        pl.semaphore_wait(hello.at[i], len(near))
        if i < 2:
            greet(hello.at[i + 1])

    barrier = pltpu.get_barrier_semaphore()
    greet(barrier)

    def load(src, dst, t, k):
        pltpu.make_async_copy(src, dst, loc_sem.at[t, k]).start()

    def loaded(t, k, o, n):
        ref = S.at[pl.ds(o, n), :]
        pltpu.make_async_copy(ref, ref, loc_sem.at[t, k]).wait()

    W2_AT, W3_AT, STAGE = 12 * D, 12 * D + 3 * H, WROWS + 3 * R

    def start_loads(t, xr, w1, w2, w3):
        o = t * STAGE

        def columns(src, at, rows, c, k):
            load(src.at[:, pl.ds(L * c, L)], S.at[pl.ds(o + at + rows * c, rows), :], t, k)
        for c in range(3):
            columns(xr, WROWS, R, c, 0)
        for c in range(12):
            columns(w1, 0, D, c, 1 + c // 4)
        for c in range(3):
            columns(w2, W2_AT, H, c, 4)
        for c in range(3):
            columns(w3, W3_AT, D, c, 5)

    start_loads(0, ix, iw1, iw2, iw3)
    load(ids_in, ids_all.at[me], 0, 6)
    load(lq_in, lq_all.at[me], 1, 6)

    def columns_of_ids():
        pltpu.make_async_copy(ids_in, ids_all.at[me], loc_sem.at[0, 6]).wait()
        pltpu.make_async_copy(lq_in, lq_all.at[me], loc_sem.at[1, 6]).wait()
        for t in range(4):
            idcol[L * t:L * t + L, :] = jnp.broadcast_to(ids_all[me, t:t + 1, :], (L, L)).T
            lqcol[L * t:L * t + L, :] = jnp.broadcast_to(lq_all[me, t:t + 1, :], (L, L)).T

    def forward(t, dest, greeting):
        o = t * STAGE

        def take(dst, at, rows, c):
            dst[t, :, L * c:L * c + L] = S[o + at + rows * c:o + at + rows * (c + 1), :].astype(BF16)

        loaded(t, 0, o + WROWS, 3 * R)
        for c in range(3):
            take(xb, WROWS, R, c)
        for n in range(3):
            loaded(t, 1 + n, o + 4 * n * D, 4 * D)
            for c in range(4):
                take(w1b, 0, D, 4 * n + c)
            cols = slice(4 * n * L, 4 * (n + 1) * L)
            h1[t, :, cols] = jnp.maximum(dot(xb[t], w1b[t, :, cols]), 0.0).astype(BF16)
        if greeting:
            greeted(0)
        loaded(t, 4, o + W2_AT, 3 * H)
        if t == 0:
            start_loads(1, ux, uw1, uw2, uw3)
        for c in range(3):
            take(w2b, W2_AT, H, c)
        h2[t] = jnp.maximum(dot(h1[t], w2b[t]), 0.0).astype(BF16)
        if greeting:
            greeted(1)
        loaded(t, 5, o + W3_AT, 3 * D)
        for c in range(3):
            take(w3b, W3_AT, D, c)
        z = dot(h2[t], w3b[t])
        inv = lax.rsqrt(jnp.sum(z * z, axis=1, keepdims=True) + EPS)
        inv_ref[t] = jnp.broadcast_to(inv, (R, L))
        e = z * inv
        e_ref[t] = e
        dest[pl.ds(pl.multiple_of(me * R, R), R), :] = e.astype(BF16)

    class Gather:
        def __init__(self, part, full, units, ssem):
            self.part, self.full, self.units, self.ssem = part, full, units, ssem
            self.rsem = new_sems(1, 7)
            self.other_sem = None

        def _each(self, rel):
            for p in range(3):
                o = [DIMS[(p + i) % 3] for i in range(3)]
                yield p, o, self.part(p, chips[sum(o[i] for i in rel)])

        def _send(self, j, pos, rel):
            for p, o, r in self._each(rel):
                send(r, r, self.ssem, self.rsem + j, nbr(o[pos]))

        def _wait(self, j):
            arrived(self.units(3), self.rsem + j)

        def _cross(self, g):
            if self.other_sem is None:
                self.other_sem = self.cross_sems()
            for m in CROSS[g]:
                for r in self.full(chips[m]):
                    send(r, r, self.ssem, self.other_sem[g], partner)

        def start(self):
            self._send(0, 0, ())
            self._send(1, 1, ())
            self._send(3, 2, ())
            self._cross(0)

        def f1w(self):
            self._wait(0)

        def f1s(self):
            self._send(2, 1, (0,))
            self._send(4, 2, (0,))

        def f1(self):
            self.f1w()
            self.f1s()

        def f2(self):
            self._wait(1)
            self._send(5, 2, (1,))

        def f2b(self):
            self._wait(3)
            self._cross(1)

        def f3(self):
            self._wait(2)
            self._send(6, 2, (0, 1))

        def f4(self):
            self._wait(4)
            self._wait(5)
            self._cross(2)

        def f5(self):
            self._wait(6)
            self._cross(3)

    class Embeddings(Gather):
        def __init__(self, buf):
            def rows(c):
                return pl.ds(pl.multiple_of((c * 2 + core) * R, R), R)
            self.buf = buf
            super().__init__(lambda p, c: buf.at[rows(c), pl.ds(L * p, L)], lambda c: (buf.at[rows(c), :],),
                             lambda n: buf.at[pl.ds(0, n // 3 * R), :], new_sems(0, 1))

        def cross_sems(self):
            k = new_sems(1, 4)
            return range(k, k + 4)

        def other(self, g):
            arrived(self.units(3 * len(CROSS[g])), self.other_sem[g])

        def finish(self):
            sent(self.units(3 * (NDEV - 1)), self.ssem)

    gv = Embeddings(v_all)
    gu = Embeddings(u_all)

    def wrow(t, p, r):
        return t * WROWS + p * PACK + r

    class Reduce(Gather):
        def __init__(self, t, piece):
            self.t, self.piece = t, piece
            self.at, self.blk = ((0, SEG // 8), (SEG, (HALF - SEG) // 8))[piece]
            self.sub = (0, SEG // 8)[piece]
            super().__init__(lambda p, c: grads.at[self.rows(p, c), :], self._all_parts,
                             lambda n: grads.at[pl.ds(0, n * self.blk), :], new_sems(0, 1))
            self.red = new_sems(1, 8)

        def rows(self, p, c):
            return pl.ds(pl.multiple_of(wrow(self.t, p, 0) + core * HALF + self.at + c * self.blk, 8), self.blk)

        def _all_parts(self, c):
            return [grads.at[self.rows(p, c), :] for p in range(3)]

        def cross_sems(self):
            return (new_sems(1, 1),) * 4

        def other(self):
            arrived(self.units(24), self.other_sem[0])

        def finish(self):
            sent(self.units(90), self.ssem)

        def cross(self):
            n = 8 * self.blk
            for p in range(3):
                rows = pl.ds(pl.multiple_of(wrow(self.t, p, 0) + (1 - core) * HALF + self.at, 8), n)
                send(S.at[rows, :], recv_d.at[p, pl.ds(self.at, n), :], self.ssem, self.red, partner)

        def _orders(self):
            for p in range(3):
                yield p, [DIMS[(p + i) % 3] for i in range(3)]

        def _got(self, k):
            arrived(self.units(3), self.red + k)

        def _buf(self, ref, *i):
            return ref.at[(*i, pl.ds(self.sub, self.blk), slice(None))]

        def _add(self, p, c, ref, *i):
            rows = self.rows(p, c)
            S[rows, :] += self._buf(ref, *i)[...]

        def _pass(self, p, c, k, dev, ref, *i):
            send(S.at[self.rows(p, c), :], self._buf(ref, *i), self.ssem, self.red + k, nbr(dev))

        def p1(self):
            arrived(self.units(24), self.red)
            for p in range(3):
                for q in range(8):
                    rows = self.rows(p, q)
                    S[rows, :] += recv_d[p, self.at + q * self.blk:self.at + (q + 1) * self.blk, :]
            if self.t == 1:
                pl.semaphore_signal(ack.at[self.piece], inc=1, device_id=(partner,), device_id_type=MESH)
            self._first(0)

        def _first(self, h):
            for s in (2 * h, 2 * h + 1):
                for p, (a, b, c) in self._orders():
                    self._pass(p, chips[a ^ (b + c, b, c, 0)[s]], 1 + s, a, rb1, p, s)

        def p1b(self):
            self._first(1)

        def p2(self):
            for s in range(2):
                self._got(1 + s)
                for p, (a, b, c) in self._orders():
                    m = (b + c, b)[s]
                    self._add(p, chips[m], rb1, p, s)
                    self._pass(p, chips[m], 5 + s, b, rb2, p, s)

        def p2b(self):
            for s in (2, 3):
                self._got(1 + s)
                for p, (a, b, c) in self._orders():
                    self._add(p, chips[(c, 0)[s - 2]], rb1, p, s)

        def p3(self):
            self._got(5)
            for p, (a, b, c) in self._orders():
                self._add(p, chips[c], rb2, p, 0)
                self._pass(p, chips[c], 7, c, rb3, p)

        def p3b(self):
            self._got(6)
            for p, (a, b, c) in self._orders():
                self._add(p, chips[0], rb2, p, 1)

        def p4(self):
            self._got(7)
            for p in range(3):
                rows = self.rows(p, chips[0])
                grads[rows, :] = S[rows, :] + self._buf(rb3, p)[...]
            self.start()

    class Push:
        def __init__(self, buf):
            self.buf, self.ssem, self.rsem = buf, new_sems(0, 1), new_sems(1, 1)

        def start(self):
            for i in range(1, NDEV):
                send(self.buf.at[me], self.buf.at[me], self.ssem, self.rsem, lax.rem(me + i, NDEV))

        def wait(self):
            arrived(self.buf.at[pl.ds(0, NDEV - 1)], self.rsem)

        def finish(self):
            sent(self.buf.at[pl.ds(0, NDEV - 1)], self.ssem)

    def order(i):
        return 4 - 2 * i + lax.div(i * (i - 1), 2)

    def device_of(slot):
        g = lax.div(slot + 1, 3)
        i = lax.rem(slot + 1, 3)
        near = order(i)
        m = jnp.where(slot < 2, 0, jnp.where(g < 3, near, jnp.where(g < 5, 7 - near, 7)))
        oth = jnp.where(slot < 2, slot, jnp.where(slot < 14, lax.rem(g - 1, 2), slot - 14))
        k = core + oth - 2 * core * oth
        return flip(m) * 2 + k

    def rowsl(q):
        return pl.ds(pl.multiple_of(q * R, R), R)

    def diag(r0, t):
        return (lax.broadcasted_iota(jnp.int32, (CH, L), 0) + r0
                == lax.broadcasted_iota(jnp.int32, (CH, L), 1) + L * t)

    def row_dot(slot):
        s512 = dot(u_all[rowsl(me), :], v_all[rowsl(device_of(slot)), :], NT)
        for t in range(4):
            S[(slot * 4 + t) * R:(slot * 4 + t + 1) * R, :] = s512[:, L * t:L * t + L]

    def row_rest(slot):
        q = device_of(slot)
        own = slot == 0
        for r0 in range(0, R, CH):
            rs = slice(r0, r0 + CH)
            idc = idcol[rs, :]
            vals = []
            pos = jnp.zeros((CH, L), F32)
            for t in range(4):
                off = slice((slot * 4 + t) * R + r0, (slot * 4 + t) * R + r0 + CH)
                s = S[off, :] * SCALE - lq_all[q, t:t + 1, :]
                hit = idc == ids_all[q, t:t + 1, :]
                if own:
                    dg = diag(r0, t)
                    pos = pos + jnp.where(dg, s, 0.0)
                    hit = jnp.logical_and(hit, jnp.logical_not(dg))
                s = jnp.where(hit, -jnp.inf, s)
                S[off, :] = s
                vals.append(s)
            mn = jnp.maximum(jnp.maximum(vals[0], vals[1]), jnp.maximum(vals[2], vals[3]))
            if own:
                pos_ref[rs, :] = pos
                mn = jnp.maximum(mn, LOWEST)
                tot = jnp.zeros((CH, L), F32)
            else:
                mo = m_ref[rs, :]
                mn = jnp.maximum(mn, mo)
                tot = l_ref[rs, :] * jnp.exp(mo - mn)
            for s in vals:
                tot = tot + jnp.exp(s - mn)
            l_ref[rs, :] = tot
            m_ref[rs, :] = mn

    def row_slots(a, b):
        row_dot(a)
        for slot in range(a, b):
            if slot + 1 < b:
                row_dot(slot + 1)
            row_rest(slot)

    def row_finish():
        m = m_ref[...]
        top = jnp.max(m, axis=1, keepdims=True)
        tot = jnp.sum(l_ref[...] * jnp.exp(m - top), axis=1, keepdims=True)
        inv = 1.0 / (tot * float(B))
        cost = top + jnp.log(tot) - jnp.sum(pos_ref[...], axis=1, keepdims=True)
        m_ref[...] = jnp.broadcast_to(top, (R, L))
        l_ref[...] = jnp.broadcast_to(inv, (R, L))
        lane = lax.broadcasted_iota(jnp.int32, (R, L), 1)
        pack = jnp.where(lane == 0, top, jnp.where(lane == 1, inv, jnp.where(lane == 2, cost, 0.0)))
        st_all[me] = pack.T[0:8, :]

    def du_fill(slot, k, own=False):
        for r0 in range(0, R, CH):
            rs = slice(r0, r0 + CH)
            mc = m_ref[rs, :]
            ic = l_ref[rs, :]
            for t in range(4):
                off = pl.ds(pl.multiple_of((slot * 4 + t) * R + r0, CH), CH)
                g = jnp.exp(S[off, :] - mc) * ic
                if own:
                    g = g - jnp.where(diag(r0, t), 1.0 / B, 0.0)
                G[k, rs, L * t:L * t + L] = g.astype(BF16)

    def du_dot(slot, k):
        acc[...] += dot(G[k], v_all[rowsl(device_of(slot)), :])

    def du_pairs(a, b):
        def pair(i, x):
            du_dot(2 * i, 0)
            du_fill(2 * i + 1, 1)
            du_dot(2 * i + 1, 1)
            du_fill(2 * i + 2, 0)
            return x
        lax.fori_loop(a, b, pair, 0)

    def dv_slot(slot, own):
        q = me if own else device_of(slot)
        big[...] = dot(v_all[rowsl(me), :], u_all[rowsl(q), :], NT)

        def chunk(r, _):
            r0 = pl.multiple_of(r * CH, CH)
            rs = pl.ds(r0, CH)
            idc = idcol[rs, :]
            lqc = lqcol[rs, :]
            for t in range(4):
                cs = slice(L * t, L * t + L)
                s = big[rs, cs] * SCALE - lqc
                hit = idc == ids_all[q, t:t + 1, :]
                if own:
                    dg = diag(r0, t)
                    hit = jnp.logical_and(hit, jnp.logical_not(dg))
                g = jnp.exp(jnp.where(hit, -jnp.inf, s) - st_all[q, 0:1, cs]) * st_all[q, 1:2, cs]
                if own:
                    g = g - jnp.where(dg, 1.0 / B, 0.0)
                G[0, rs, cs] = g.astype(BF16)
            return 0
        lax.fori_loop(0, R // CH, chunk, 0)
        part = dot(G[0], u_all[rowsl(q), :])
        acc[...] = part if own else acc[...] + part

    def dv_slots(a, b):
        lax.fori_loop(a, b, lambda s, c: (dv_slot(s, False), c)[1], 0)

    def put(t, r0, val):
        n = val.shape[0]
        for p in range(3):
            S[pl.ds(pl.multiple_of(wrow(t, p, 0) + r0, 8), n), :] = val[:, L * p:L * p + L]

    def backward(t, reds, hooks):
        d = acc[...] * SCALE
        e = e_ref[t]
        inv = inv_ref[t]
        s = jnp.sum(e * d, axis=1, keepdims=True)
        dzb = ((d - e * s) * jnp.concatenate([inv, inv, inv], axis=1)).astype(BF16)
        g3 = dot(h2[t], dzb, TN)
        put(t, 2 * D, g3[:D // 2])
        put(t, HALF + 2 * D, g3[D // 2:])
        da2 = jnp.where(h2[t] > 0, dot(dzb, w3b[t], NT), 0.0).astype(BF16)
        G[0, :, 0:D] = da2

        def mid(i):
            c = lax.rem(i + 2 * (1 - core), 4)
            base = lax.div(c, 2) * HALF + lax.rem(c, 2) * SEG
            cols = pl.ds(pl.multiple_of(c * D, L), D)
            g2 = G[0, :, 0:D]
            put(t, base, dot(h1[t, :, cols], g2, TN))
            g1 = dot(g2, w2b[t, cols, :], NT)
            da1[...] = jnp.where(h1[t, :, cols] > 0, g1, 0.0).astype(BF16)
            put(t, base + D, dot(xb[t], da1[...], TN))

        hooks[0]()
        mid(0)
        hooks[1]()
        reds[0].cross()
        mid(1)
        hooks[2]()
        reds[1].cross()
        lax.fori_loop(2, 4, lambda i, x: (mid(i), x)[1], 0)

    pi, pq, ps = Push(ids_all), Push(lq_all), Push(st_all)
    ua, ub, ia, ib = Reduce(1, 0), Reduce(1, 1), Reduce(0, 0), Reduce(0, 1)

    def nothing():
        pass

    forward(0, v_all, False)
    pl.semaphore_wait(barrier, len(near))
    gv.start()
    greet(hello.at[0])
    columns_of_ids()
    forward(1, u_all, True)
    greeted(2)
    pi.start()
    pq.start()
    gv.f1()
    pi.wait()
    pq.wait()
    gv.other(0)
    row_slots(0, 2)
    gv.f2()
    gv.f2b()
    row_slots(2, 5)
    gv.f3()
    gu.start()
    gv.other(1)
    row_slots(5, 8)
    gv.f4()
    row_slots(8, 11)
    gv.f5()
    gv.other(2)
    row_slots(11, 15)
    gv.other(3)
    row_slots(15, 16)
    gu.f1()
    row_finish()
    ps.start()
    gu.f2()
    acc[...] = jnp.zeros((R, D), F32)
    du_fill(0, 0, True)
    du_pairs(0, 3)
    gu.f2b()
    du_pairs(3, 7)
    du_dot(14, 0)
    du_fill(15, 1)
    du_dot(15, 1)
    backward(1, (ua, ub), (nothing, gu.f3, nothing))
    ua.p1()
    ua.p1b()
    ub.p1()
    gu.f4()
    ps.wait()
    gu.other(0)
    gu.other(1)
    dv_slot(0, True)
    dv_slots(1, 4)
    ua.p2()
    ub.p1b()
    gu.f5()
    dv_slots(4, 6)
    ua.p2b()
    gu.other(2)
    dv_slots(6, 9)
    ua.p3()
    ub.p2()
    dv_slots(9, 10)
    ua.p3b()
    gu.other(3)
    dv_slots(10, 11)
    ub.p2b()
    dv_slots(11, 12)
    ua.p4()
    dv_slots(12, 13)
    ub.p3()
    dv_slots(13, 15)
    ub.p3b()
    dv_slots(15, 16)
    ub.p4()

    def turn(i):
        def go():
            if i == 0:
                ua.f1()
            pl.semaphore_wait(ack.at[i], 1)
        return go

    backward(0, (ia, ib), (nothing, turn(0), turn(1)))
    ia.p1()
    ia.p1b()
    ub.f1w()
    ib.p1()
    ib.p1b()
    ia.p2()
    ib.p2()
    ua.f2()
    ia.p2b()
    ia.p3()
    ub.f1s()
    ub.f2()
    ib.p2b()
    ia.p3b()
    ib.p3()
    ua.f2b()
    ua.f3()
    ia.p4()
    ib.p3b()
    ub.f2b()
    ub.f3()
    ib.p4()
    ua.f4()
    ub.f4()
    ua.f5()
    ub.f5()
    total = jnp.sum(jnp.sum(st_all[...], axis=0)[2:3, :]) * (1.0 / B)
    loss[0, 0] = total
    ia.f1()
    ia.f2()
    ib.f1()
    ib.f2()
    ua.other()
    ub.other()
    ia.f2b()
    ia.f3()
    ib.f2b()
    ib.f3()
    ia.f4()
    ib.f4()
    ia.f5()
    ib.f5()
    ia.other()
    ib.other()
    for x in (gv, gu, pi, pq, ps, ua, ub, ia, ib):
        x.finish()


def write_kernel(loss_in, grads, loss, gu1, gu2, gu3, gi1, gi2, gi3, sem):
    loss[0, 0] = loss_in[0, 0]
    for t, (g1, g2, g3) in enumerate(((gi1, gi2, gi3), (gu1, gu2, gu3))):
        for p in range(3):
            pc = pl.ds(L * p, L)
            for h in range(2):
                o = t * WROWS + p * PACK + h * HALF
                jobs = [(o + 2 * D, g3.at[pl.ds(h * (D // 2), D // 2), pc])]
                for i in range(2):
                    c = 2 * h + i
                    jobs.append((o + i * SEG, g2.at[pl.ds(D * c, D), pc]))
                    jobs.append((o + i * SEG + D, g1.at[:, pl.ds(D * c + L * p, L)]))
                for r0, dst in jobs:
                    src = grads.at[pl.ds(r0, dst.shape[0]), :]
                    pltpu.make_async_copy(src, dst, sem).start()
    pltpu.make_async_copy(grads, grads, sem).wait()


def solution(mesh):
    vm = pl.BlockSpec(memory_space=pltpu.VMEM)
    sm = pl.BlockSpec(memory_space=pltpu.SMEM)
    hbm = pl.BlockSpec(memory_space=pl.ANY)
    shp = jax.ShapeDtypeStruct

    def device_step(user_x, item_x, item_id, log_q, user_w1, user_w2, user_w3, item_w1, item_w2, item_w3):
        V = pltpu.VMEM
        loss, grads = pl.pallas_call(
            kernel,
            out_shape=(shp((1, 1), F32), V((2 * WROWS, L), F32)),
            in_specs=[hbm] * 10,
            out_specs=(sm, vm),
            scratch_shapes=[
                V((64 * R, L), F32), V((B, D), BF16), V((B, D), BF16),
                V((2, R, D), BF16), V((2, R, H), BF16), V((2, R, D), BF16),
                V((2, R, D), F32), V((2, R, L), F32),
                V((2, D, H), BF16), V((2, H, D), BF16), V((2, D, D), BF16), V((R, D), BF16),
                V((NDEV, 4, L), jnp.int32), V((NDEV, 4, L), F32), V((NDEV, 8, R), F32),
                V((R, L), jnp.int32), V((R, L), F32), V((R, L), F32), V((R, L), F32), V((R, L), F32),
                V((2, R, R), BF16), V((R, D), F32), V((R, R), F32),
                V((3, HALF, L), F32), V((3, 4, BLK, L), F32), V((3, 2, BLK, L), F32),
                V((3, BLK, L), F32),
                pltpu.SemaphoreType.DMA((N_SEND,)), pltpu.SemaphoreType.DMA((N_RECV,)),
                pltpu.SemaphoreType.DMA((2, 7)), pltpu.SemaphoreType.REGULAR((2,)),
                pltpu.SemaphoreType.REGULAR((3,)),
            ],
            compiler_params=pltpu.CompilerParams(collective_id=0, has_side_effects=True,
                                                 vmem_limit_bytes=VMEM_LIMIT),
            name='step',
        )(user_x, item_x, item_id.reshape(4, L), log_q.reshape(4, L),
          user_w1, user_w2, user_w3, item_w1, item_w2, item_w3)
        out = pl.pallas_call(
            write_kernel,
            out_shape=(shp((1, 1), F32), shp((D, H), F32), shp((H, D), F32), shp((D, D), F32),
                       shp((D, H), F32), shp((H, D), F32), shp((D, D), F32)),
            in_specs=[sm, vm],
            out_specs=(sm,) + (hbm,) * 6,
            scratch_shapes=[pltpu.SemaphoreType.DMA],
            compiler_params=pltpu.CompilerParams(vmem_limit_bytes=1 << 20),
            name='write',
        )(loss, grads)
        return (out[0].reshape(()),) + tuple(out[1:])

    batch_spec = P('dp', None)
    vec_spec = P('dp')
    whole = P()
    return jax.shard_map(device_step, mesh=mesh,
                         in_specs=(batch_spec, batch_spec, vec_spec, vec_spec, whole, whole, whole, whole, whole, whole),
                         out_specs=(whole,) * 7, check_vma=False)
```

```python
import jax
import jax.numpy as jnp
from jax import lax
from jax.experimental import pallas as pl
from jax.experimental.pallas import tpu as pltpu
from jax.sharding import PartitionSpec as P

SCALE = 20.0
EPS = 1e-6
NDEV = 16
R = 512
D = 384
H = 1536
B = R * NDEV
BLK = 216
HALF = 8 * BLK
N_SEND, N_RECV = 9, 73
PACK = 2 * HALF
SEG = 960
WROWS = 3 * PACK
L = 128
CH = 64
VMEM_LIMIT = 56000000
F32, BF16 = jnp.float32, jnp.bfloat16
MESH = pl.DeviceIdType.MESH
NT = (((1,), (1,)), ((), ()))
TN = (((0,), (0,)), ((), ()))
LOWEST = float(jnp.finfo(jnp.float32).min)
DIMS = (4, 2, 1)
CROSS = ((0,), (4, 2, 1), (6, 5, 3), (7,))


def dot(a, b, dims=(((1,), (0,)), ((), ()))):
    return lax.dot_general(a, b, dims, preferred_element_type=F32)


def kernel(ux, ix, ids_in, lq_in, uw1, uw2, uw3, iw1, iw2, iw3,
           loss, grads,
           S, v_all, u_all, xb, h1, h2, e_ref, inv_ref, w1b, w2b, w3b, da1,
           ids_all, lq_all, st_all, idcol, lqcol, m_ref, l_ref, pos_ref, G, acc, big,
           recv_d, rb1, rb2, rb3, send_sem, recv_sem, loc_sem, ack, hello):
    made = [0, 0]

    def new_sems(kind, n):
        made[kind] += n
        return made[kind] - n

    me = lax.axis_index('dp')
    core = lax.rem(me, 2)
    chip = lax.div(me, 2)
    partner = me + 1 - 2 * core

    def flip(m):
        out = 0
        for d in DIMS:
            bit = lax.rem(lax.div(chip, d), 2)
            if isinstance(m, int):
                f = (m // d) % 2
            else:
                f = lax.rem(lax.div(m, d), 2)
            out = out + d * (bit + f - 2 * bit * f)
        return out

    chips = [flip(m) for m in range(8)]

    def nbr(d):
        return chips[d] * 2 + core

    def rc(src, dst, ssem, rsem, dev):
        return pltpu.make_async_remote_copy(src, dst, send_sem.at[ssem], recv_sem.at[rsem],
                                            device_id=(dev,), device_id_type=MESH)

    def send(src, dst, ssem, rsem, dev):
        rc(src, dst, ssem, rsem, dev).start()

    def arrived(ref, rsem):
        rc(ref, ref, 0, rsem, partner).wait_recv()

    def sent(ref, ssem):
        rc(ref, ref, ssem, 0, partner).wait_send()

    near = [partner] + [nbr(d) for d in DIMS]

    def greet(sem):
        for n in near:
            pl.semaphore_signal(sem, inc=1, device_id=(n,), device_id_type=MESH)

    def greeted(i):
        pl.semaphore_wait(hello.at[i], len(near))
        if i < 2:
            greet(hello.at[i + 1])

    barrier = pltpu.get_barrier_semaphore()
    greet(barrier)

    def load(src, dst, t, k):
        pltpu.make_async_copy(src, dst, loc_sem.at[t, k]).start()

    def loaded(t, k, o, n):
        ref = S.at[pl.ds(o, n), :]
        pltpu.make_async_copy(ref, ref, loc_sem.at[t, k]).wait()

    W2_AT, W3_AT, STAGE = 12 * D, 12 * D + 3 * H, WROWS + 3 * R

    def start_loads(t, xr, w1, w2, w3):
        o = t * STAGE

        def columns(src, at, rows, c, k):
            load(src.at[:, pl.ds(L * c, L)], S.at[pl.ds(o + at + rows * c, rows), :], t, k)
        for c in range(3):
            columns(xr, WROWS, R, c, 0)
        for c in range(12):
            columns(w1, 0, D, c, 1 + c // 4)
        for c in range(3):
            columns(w2, W2_AT, H, c, 4)
        for c in range(3):
            columns(w3, W3_AT, D, c, 5)

    start_loads(0, ix, iw1, iw2, iw3)
    load(ids_in, ids_all.at[me], 0, 6)
    load(lq_in, lq_all.at[me], 1, 6)

    def columns_of_ids():
        pltpu.make_async_copy(ids_in, ids_all.at[me], loc_sem.at[0, 6]).wait()
        pltpu.make_async_copy(lq_in, lq_all.at[me], loc_sem.at[1, 6]).wait()
        for t in range(4):
            idcol[L * t:L * t + L, :] = jnp.broadcast_to(ids_all[me, t:t + 1, :], (L, L)).T
            lqcol[L * t:L * t + L, :] = jnp.broadcast_to(lq_all[me, t:t + 1, :], (L, L)).T

    def forward(t, dest, greeting):
        o = t * STAGE

        def take(dst, at, rows, c):
            dst[t, :, L * c:L * c + L] = S[o + at + rows * c:o + at + rows * (c + 1), :].astype(BF16)

        loaded(t, 0, o + WROWS, 3 * R)
        for c in range(3):
            take(xb, WROWS, R, c)
        for n in range(3):
            loaded(t, 1 + n, o + 4 * n * D, 4 * D)
            for c in range(4):
                take(w1b, 0, D, 4 * n + c)
            cols = slice(4 * n * L, 4 * (n + 1) * L)
            h1[t, :, cols] = jnp.maximum(dot(xb[t], w1b[t, :, cols]), 0.0).astype(BF16)
        if greeting:
            greeted(0)
        loaded(t, 4, o + W2_AT, 3 * H)
        if t == 0:
            start_loads(1, ux, uw1, uw2, uw3)
        for c in range(3):
            take(w2b, W2_AT, H, c)
        h2[t] = jnp.maximum(dot(h1[t], w2b[t]), 0.0).astype(BF16)
        if greeting:
            greeted(1)
        loaded(t, 5, o + W3_AT, 3 * D)
        for c in range(3):
            take(w3b, W3_AT, D, c)
        z = dot(h2[t], w3b[t])
        inv = lax.rsqrt(jnp.sum(z * z, axis=1, keepdims=True) + EPS)
        inv_ref[t] = jnp.broadcast_to(inv, (R, L))
        e = z * inv
        e_ref[t] = e
        dest[pl.ds(pl.multiple_of(me * R, R), R), :] = e.astype(BF16)

    class Gather:
        def __init__(self, part, full, units, ssem):
            self.part, self.full, self.units, self.ssem = part, full, units, ssem
            self.rsem = new_sems(1, 7)
            self.other_sem = None

        def _each(self, rel):
            for p in range(3):
                o = [DIMS[(p + i) % 3] for i in range(3)]
                yield p, o, self.part(p, chips[sum(o[i] for i in rel)])

        def _send(self, j, pos, rel):
            for p, o, r in self._each(rel):
                send(r, r, self.ssem, self.rsem + j, nbr(o[pos]))

        def _wait(self, j):
            arrived(self.units(3), self.rsem + j)

        def _cross(self, g):
            if self.other_sem is None:
                self.other_sem = self.cross_sems()
            for m in CROSS[g]:
                for r in self.full(chips[m]):
                    send(r, r, self.ssem, self.other_sem[g], partner)

        def start(self):
            self._send(0, 0, ())
            self._send(1, 1, ())
            self._send(3, 2, ())
            self._cross(0)

        def f1w(self):
            self._wait(0)

        def f1s(self):
            self._send(2, 1, (0,))
            self._send(4, 2, (0,))

        def f1(self):
            self.f1w()
            self.f1s()

        def f2(self):
            self._wait(1)
            self._send(5, 2, (1,))

        def f2b(self):
            self._wait(3)
            self._cross(1)

        def f3(self):
            self._wait(2)
            self._send(6, 2, (0, 1))

        def f4(self):
            self._wait(4)
            self._wait(5)
            self._cross(2)

        def f5(self):
            self._wait(6)
            self._cross(3)

    class Embeddings(Gather):
        def __init__(self, buf):
            def rows(c):
                return pl.ds(pl.multiple_of((c * 2 + core) * R, R), R)
            self.buf = buf
            super().__init__(lambda p, c: buf.at[rows(c), pl.ds(L * p, L)], lambda c: (buf.at[rows(c), :],),
                             lambda n: buf.at[pl.ds(0, n // 3 * R), :], new_sems(0, 1))

        def cross_sems(self):
            k = new_sems(1, 4)
            return range(k, k + 4)

        def other(self, g):
            arrived(self.units(3 * len(CROSS[g])), self.other_sem[g])

        def finish(self):
            sent(self.units(3 * (NDEV - 1)), self.ssem)

    gv = Embeddings(v_all)
    gu = Embeddings(u_all)

    def wrow(t, p, r):
        return t * WROWS + p * PACK + r

    class Reduce(Gather):
        def __init__(self, t, piece, other=None):
            self.t, self.piece = t, piece
            self.at, self.blk = ((0, SEG // 8), (SEG, (HALF - SEG) // 8))[piece]
            self.sub = (0, SEG // 8)[piece]
            super().__init__(lambda p, c: grads.at[self.rows(p, c), :], self._all_parts,
                             lambda n: grads.at[pl.ds(0, n * self.blk), :], new_sems(0, 1))
            self.red = new_sems(1, 8) if other is None else other.red

        def rows(self, p, c):
            return pl.ds(pl.multiple_of(wrow(self.t, p, 0) + core * HALF + self.at + c * self.blk, 8), self.blk)

        def _all_parts(self, c):
            return [grads.at[self.rows(p, c), :] for p in range(3)]

        def cross_sems(self):
            return (new_sems(1, 1),) * 4

        def other(self):
            arrived(self.units(24), self.other_sem[0])

        def finish(self):
            sent(self.units(90), self.ssem)

        def cross(self):
            n = 8 * self.blk
            for p in range(3):
                rows = pl.ds(pl.multiple_of(wrow(self.t, p, 0) + (1 - core) * HALF + self.at, 8), n)
                send(S.at[rows, :], recv_d.at[p, pl.ds(self.at, n), :], self.ssem, self.red, partner)

        def _orders(self):
            for p in range(3):
                yield p, [DIMS[(p + i) % 3] for i in range(3)]

        def _got(self, k):
            arrived(self.units(3), self.red + k)

        def _buf(self, ref, *i):
            return ref.at[(*i, pl.ds(self.sub, self.blk), slice(None))]

        def _add(self, p, c, ref, *i):
            rows = self.rows(p, c)
            S[rows, :] += self._buf(ref, *i)[...]

        def _pass(self, p, c, k, dev, ref, *i):
            send(S.at[self.rows(p, c), :], self._buf(ref, *i), self.ssem, self.red + k, nbr(dev))

        def p1(self):
            arrived(self.units(24), self.red)
            for p in range(3):
                for q in range(8):
                    rows = self.rows(p, q)
                    S[rows, :] += recv_d[p, self.at + q * self.blk:self.at + (q + 1) * self.blk, :]
            if self.t == 1:
                pl.semaphore_signal(ack.at[self.piece], inc=1, device_id=(partner,), device_id_type=MESH)
            self._first(0)

        def _first(self, h):
            for s in (2 * h, 2 * h + 1):
                for p, (a, b, c) in self._orders():
                    self._pass(p, chips[a ^ (b + c, b, c, 0)[s]], 1 + s, a, rb1, p, s)

        def p1b(self):
            self._first(1)

        def p2(self):
            for s in range(2):
                self._got(1 + s)
                for p, (a, b, c) in self._orders():
                    m = (b + c, b)[s]
                    self._add(p, chips[m], rb1, p, s)
                    self._pass(p, chips[m], 5 + s, b, rb2, p, s)

        def p2b(self):
            for s in (2, 3):
                self._got(1 + s)
                for p, (a, b, c) in self._orders():
                    self._add(p, chips[(c, 0)[s - 2]], rb1, p, s)

        def p3(self):
            self._got(5)
            for p, (a, b, c) in self._orders():
                self._add(p, chips[c], rb2, p, 0)
                self._pass(p, chips[c], 7, c, rb3, p)

        def p3b(self):
            self._got(6)
            for p, (a, b, c) in self._orders():
                self._add(p, chips[0], rb2, p, 1)

        def p4(self):
            self._got(7)
            for p in range(3):
                rows = self.rows(p, chips[0])
                grads[rows, :] = S[rows, :] + self._buf(rb3, p)[...]
            self.start()

    class Push:
        def __init__(self, buf):
            self.buf, self.ssem, self.rsem = buf, new_sems(0, 1), new_sems(1, 1)

        def start(self):
            for i in range(1, NDEV):
                send(self.buf.at[me], self.buf.at[me], self.ssem, self.rsem, lax.rem(me + i, NDEV))

        def wait(self):
            arrived(self.buf.at[pl.ds(0, NDEV - 1)], self.rsem)

        def finish(self):
            sent(self.buf.at[pl.ds(0, NDEV - 1)], self.ssem)

    def order(i):
        return 4 - 2 * i + lax.div(i * (i - 1), 2)

    def device_of(slot):
        g = lax.div(slot + 1, 3)
        i = lax.rem(slot + 1, 3)
        near = order(i)
        m = jnp.where(slot < 2, 0, jnp.where(g < 3, near, jnp.where(g < 5, 7 - near, 7)))
        oth = jnp.where(slot < 2, slot, jnp.where(slot < 14, lax.rem(g - 1, 2), slot - 14))
        k = core + oth - 2 * core * oth
        return flip(m) * 2 + k

    def rowsl(q):
        return pl.ds(pl.multiple_of(q * R, R), R)

    def diag(r0, t):
        return (lax.broadcasted_iota(jnp.int32, (CH, L), 0) + r0
                == lax.broadcasted_iota(jnp.int32, (CH, L), 1) + L * t)

    def row_dot(slot):
        s512 = dot(u_all[rowsl(me), :], v_all[rowsl(device_of(slot)), :], NT)
        for t in range(4):
            S[(slot * 4 + t) * R:(slot * 4 + t + 1) * R, :] = s512[:, L * t:L * t + L]

    def row_rest(slot):
        q = device_of(slot)
        own = slot == 0
        for r0 in range(0, R, CH):
            rs = slice(r0, r0 + CH)
            idc = idcol[rs, :]
            vals = []
            pos = jnp.zeros((CH, L), F32)
            for t in range(4):
                off = slice((slot * 4 + t) * R + r0, (slot * 4 + t) * R + r0 + CH)
                s = S[off, :] * SCALE - lq_all[q, t:t + 1, :]
                hit = idc == ids_all[q, t:t + 1, :]
                if own:
                    dg = diag(r0, t)
                    pos = pos + jnp.where(dg, s, 0.0)
                    hit = jnp.logical_and(hit, jnp.logical_not(dg))
                s = jnp.where(hit, -jnp.inf, s)
                S[off, :] = s
                vals.append(s)
            mn = jnp.maximum(jnp.maximum(vals[0], vals[1]), jnp.maximum(vals[2], vals[3]))
            if own:
                pos_ref[rs, :] = pos
                mn = jnp.maximum(mn, LOWEST)
                tot = jnp.zeros((CH, L), F32)
            else:
                mo = m_ref[rs, :]
                mn = jnp.maximum(mn, mo)
                tot = l_ref[rs, :] * jnp.exp(mo - mn)
            for s in vals:
                tot = tot + jnp.exp(s - mn)
            l_ref[rs, :] = tot
            m_ref[rs, :] = mn

    def row_slots(a, b):
        row_dot(a)
        for slot in range(a, b):
            if slot + 1 < b:
                row_dot(slot + 1)
            row_rest(slot)

    def row_finish():
        m = m_ref[...]
        top = jnp.max(m, axis=1, keepdims=True)
        tot = jnp.sum(l_ref[...] * jnp.exp(m - top), axis=1, keepdims=True)
        inv = 1.0 / (tot * float(B))
        cost = top + jnp.log(tot) - jnp.sum(pos_ref[...], axis=1, keepdims=True)
        m_ref[...] = jnp.broadcast_to(top, (R, L))
        l_ref[...] = jnp.broadcast_to(inv, (R, L))
        lane = lax.broadcasted_iota(jnp.int32, (R, L), 1)
        pack = jnp.where(lane == 0, top, jnp.where(lane == 1, inv, jnp.where(lane == 2, cost, 0.0)))
        st_all[me] = pack.T[0:8, :]

    def du_fill(slot, k, own=False):
        for r0 in range(0, R, CH):
            rs = slice(r0, r0 + CH)
            mc = m_ref[rs, :]
            ic = l_ref[rs, :]
            for t in range(4):
                off = pl.ds(pl.multiple_of((slot * 4 + t) * R + r0, CH), CH)
                g = jnp.exp(S[off, :] - mc) * ic
                if own:
                    g = g - jnp.where(diag(r0, t), 1.0 / B, 0.0)
                G[k, rs, L * t:L * t + L] = g.astype(BF16)

    def du_dot(slot, k):
        acc[...] += dot(G[k], v_all[rowsl(device_of(slot)), :])

    def du_pairs(a, b):
        def pair(i, x):
            du_dot(2 * i, 0)
            du_fill(2 * i + 1, 1)
            du_dot(2 * i + 1, 1)
            du_fill(2 * i + 2, 0)
            return x
        lax.fori_loop(a, b, pair, 0)

    def dv_slot(slot, own):
        q = me if own else device_of(slot)
        big[...] = dot(v_all[rowsl(me), :], u_all[rowsl(q), :], NT)

        def chunk(r, _):
            r0 = pl.multiple_of(r * CH, CH)
            rs = pl.ds(r0, CH)
            idc = idcol[rs, :]
            lqc = lqcol[rs, :]
            for t in range(4):
                cs = slice(L * t, L * t + L)
                s = big[rs, cs] * SCALE - lqc
                hit = idc == ids_all[q, t:t + 1, :]
                if own:
                    dg = diag(r0, t)
                    hit = jnp.logical_and(hit, jnp.logical_not(dg))
                g = jnp.exp(jnp.where(hit, -jnp.inf, s) - st_all[q, 0:1, cs]) * st_all[q, 1:2, cs]
                if own:
                    g = g - jnp.where(dg, 1.0 / B, 0.0)
                G[0, rs, cs] = g.astype(BF16)
            return 0
        lax.fori_loop(0, R // CH, chunk, 0)
        part = dot(G[0], u_all[rowsl(q), :])
        acc[...] = part if own else acc[...] + part

    def dv_slots(a, b):
        lax.fori_loop(a, b, lambda s, c: (dv_slot(s, False), c)[1], 0)

    def put(t, r0, val):
        n = val.shape[0]
        for p in range(3):
            S[pl.ds(pl.multiple_of(wrow(t, p, 0) + r0, 8), n), :] = val[:, L * p:L * p + L]

    def backward(t, reds, hooks):
        d = acc[...] * SCALE
        e = e_ref[t]
        inv = inv_ref[t]
        s = jnp.sum(e * d, axis=1, keepdims=True)
        dzb = ((d - e * s) * jnp.concatenate([inv, inv, inv], axis=1)).astype(BF16)
        g3 = dot(h2[t], dzb, TN)
        put(t, 2 * D, g3[:D // 2])
        put(t, HALF + 2 * D, g3[D // 2:])
        da2 = jnp.where(h2[t] > 0, dot(dzb, w3b[t], NT), 0.0).astype(BF16)
        G[0, :, 0:D] = da2

        def mid(i):
            c = lax.rem(i + 2 * (1 - core), 4)
            base = lax.div(c, 2) * HALF + lax.rem(c, 2) * SEG
            cols = pl.ds(pl.multiple_of(c * D, L), D)
            g2 = G[0, :, 0:D]
            put(t, base, dot(h1[t, :, cols], g2, TN))
            g1 = dot(g2, w2b[t, cols, :], NT)
            da1[...] = jnp.where(h1[t, :, cols] > 0, g1, 0.0).astype(BF16)
            put(t, base + D, dot(xb[t], da1[...], TN))

        hooks[0]()
        mid(0)
        hooks[1]()
        reds[0].cross()
        mid(1)
        hooks[2]()
        reds[1].cross()
        lax.fori_loop(2, 4, lambda i, x: (mid(i), x)[1], 0)

    pi, pq, ps = Push(ids_all), Push(lq_all), Push(st_all)
    ua, ub = Reduce(1, 0), Reduce(1, 1)
    ia, ib = Reduce(0, 0, ua), Reduce(0, 1, ub)

    def nothing():
        pass

    forward(0, v_all, False)
    pl.semaphore_wait(barrier, len(near))
    gv.start()
    greet(hello.at[0])
    columns_of_ids()
    forward(1, u_all, True)
    greeted(2)
    pi.start()
    pq.start()
    gv.f1()
    pi.wait()
    pq.wait()
    gv.other(0)
    row_slots(0, 2)
    gv.f2()
    gv.f2b()
    row_slots(2, 5)
    gv.f3()
    gu.start()
    gv.other(1)
    row_slots(5, 8)
    gv.f4()
    row_slots(8, 11)
    gv.f5()
    gv.other(2)
    row_slots(11, 15)
    gv.other(3)
    row_slots(15, 16)
    gu.f1()
    row_finish()
    ps.start()
    gu.f2()
    acc[...] = jnp.zeros((R, D), F32)
    du_fill(0, 0, True)
    du_pairs(0, 3)
    gu.f2b()
    du_pairs(3, 7)
    du_dot(14, 0)
    du_fill(15, 1)
    du_dot(15, 1)
    backward(1, (ua, ub), (nothing, gu.f3, nothing))
    ua.p1()
    ua.p1b()
    ub.p1()
    gu.f4()
    ps.wait()
    gu.other(0)
    gu.other(1)
    dv_slot(0, True)
    dv_slots(1, 4)
    ua.p2()
    ub.p1b()
    gu.f5()
    dv_slots(4, 6)
    ua.p2b()
    gu.other(2)
    dv_slots(6, 9)
    ua.p3()
    ub.p2()
    dv_slots(9, 10)
    ua.p3b()
    gu.other(3)
    dv_slots(10, 11)
    ub.p2b()
    dv_slots(11, 12)
    ua.p4()
    dv_slots(12, 13)
    ub.p3()
    dv_slots(13, 15)
    ub.p3b()
    dv_slots(15, 16)
    ub.p4()

    def turn(i):
        def go():
            if i == 0:
                ua.f1()
            pl.semaphore_wait(ack.at[i], 1)
        return go

    backward(0, (ia, ib), (nothing, turn(0), turn(1)))
    ia.p1()
    ia.p1b()
    ub.f1w()
    ib.p1()
    ib.p1b()
    ia.p2()
    ib.p2()
    ua.f2()
    ia.p2b()
    ia.p3()
    ub.f1s()
    ub.f2()
    ib.p2b()
    ia.p3b()
    ib.p3()
    ua.f2b()
    ua.f3()
    ia.p4()
    ib.p3b()
    ub.f2b()
    ub.f3()
    ib.p4()
    ua.f4()
    ub.f4()
    ua.f5()
    ub.f5()
    total = jnp.sum(jnp.sum(st_all[...], axis=0)[2:3, :]) * (1.0 / B)
    loss[0, 0] = total
    ia.f1()
    ia.f2()
    ib.f1()
    ib.f2()
    ua.other()
    ub.other()
    ia.f2b()
    ia.f3()
    ib.f2b()
    ib.f3()
    ia.f4()
    ib.f4()
    ia.f5()
    ib.f5()
    ia.other()
    ib.other()
    for x in (gv, gu, pi, pq, ps, ua, ub, ia, ib):
        x.finish()


def write_kernel(loss_in, grads, loss, gu1, gu2, gu3, gi1, gi2, gi3, sem):
    loss[0, 0] = loss_in[0, 0]
    for t, (g1, g2, g3) in enumerate(((gi1, gi2, gi3), (gu1, gu2, gu3))):
        for p in range(3):
            pc = pl.ds(L * p, L)
            for h in range(2):
                o = t * WROWS + p * PACK + h * HALF
                jobs = [(o + 2 * D, g3.at[pl.ds(h * (D // 2), D // 2), pc])]
                for i in range(2):
                    c = 2 * h + i
                    jobs.append((o + i * SEG, g2.at[pl.ds(D * c, D), pc]))
                    jobs.append((o + i * SEG + D, g1.at[:, pl.ds(D * c + L * p, L)]))
                for r0, dst in jobs:
                    src = grads.at[pl.ds(r0, dst.shape[0]), :]
                    pltpu.make_async_copy(src, dst, sem).start()
    pltpu.make_async_copy(grads, grads, sem).wait()


def solution(mesh):
    vm = pl.BlockSpec(memory_space=pltpu.VMEM)
    sm = pl.BlockSpec(memory_space=pltpu.SMEM)
    hbm = pl.BlockSpec(memory_space=pl.ANY)
    shp = jax.ShapeDtypeStruct

    def device_step(user_x, item_x, item_id, log_q, user_w1, user_w2, user_w3, item_w1, item_w2, item_w3):
        V = pltpu.VMEM
        loss, grads = pl.pallas_call(
            kernel,
            out_shape=(shp((1, 1), F32), V((2 * WROWS, L), F32)),
            in_specs=[hbm] * 10,
            out_specs=(sm, vm),
            scratch_shapes=[
                V((64 * R, L), F32), V((B, D), BF16), V((B, D), BF16),
                V((2, R, D), BF16), V((2, R, H), BF16), V((2, R, D), BF16),
                V((2, R, D), F32), V((2, R, L), F32),
                V((2, D, H), BF16), V((2, H, D), BF16), V((2, D, D), BF16), V((R, D), BF16),
                V((NDEV, 4, L), jnp.int32), V((NDEV, 4, L), F32), V((NDEV, 8, R), F32),
                V((R, L), jnp.int32), V((R, L), F32), V((R, L), F32), V((R, L), F32), V((R, L), F32),
                V((2, R, R), BF16), V((R, D), F32), V((R, R), F32),
                V((3, HALF, L), F32), V((3, 4, BLK, L), F32), V((3, 2, BLK, L), F32),
                V((3, BLK, L), F32),
                pltpu.SemaphoreType.DMA((N_SEND,)), pltpu.SemaphoreType.DMA((N_RECV,)),
                pltpu.SemaphoreType.DMA((2, 7)), pltpu.SemaphoreType.REGULAR((2,)),
                pltpu.SemaphoreType.REGULAR((3,)),
            ],
            compiler_params=pltpu.CompilerParams(collective_id=0, has_side_effects=True,
                                                 vmem_limit_bytes=VMEM_LIMIT),
            name='step',
        )(user_x, item_x, item_id.reshape(4, L), log_q.reshape(4, L),
          user_w1, user_w2, user_w3, item_w1, item_w2, item_w3)
        out = pl.pallas_call(
            write_kernel,
            out_shape=(shp((1, 1), F32), shp((D, H), F32), shp((H, D), F32), shp((D, D), F32),
                       shp((D, H), F32), shp((H, D), F32), shp((D, D), F32)),
            in_specs=[sm, vm],
            out_specs=(sm,) + (hbm,) * 6,
            scratch_shapes=[pltpu.SemaphoreType.DMA],
            compiler_params=pltpu.CompilerParams(vmem_limit_bytes=1 << 20),
            name='write',
        )(loss, grads)
        return (out[0].reshape(()),) + tuple(out[1:])

    batch_spec = P('dp', None)
    vec_spec = P('dp')
    whole = P()
    return jax.shard_map(device_step, mesh=mesh,
                         in_specs=(batch_spec, batch_spec, vec_spec, vec_spec, whole, whole, whole, whole, whole, whole),
                         out_specs=(whole,) * 7, check_vma=False)
```
